8 devices in a mesh: dp: 2 (over y, z), sp: 4 (over x, core).
Axes of the slice: x: 2, y: 2, z: 1, core: 2. Of those that a mesh axis runs over, the one named last changes fastest.
Arguments:
- x: bfloat16 [8192, 1024], P(('dp', 'sp')), parts along dimension 0
- gain: bfloat16 [1024], replicated
- wq: bfloat16 [1024, 4096], P('sp')
- wk: bfloat16 [1024, 4096], P('sp')
- wv: bfloat16 [1024, 4096], P('sp')
- wo: bfloat16 [4096, 1024], P('sp')
Outputs:
- output: bfloat16 [8192, 1024], P(('dp', 'sp')), parts along dimension 0
There are 2 independent parts. The reference program is written for one: setup_inputs(seed, part) draws one part's arguments, and reference() takes and returns one part's arrays. A program takes and returns all parts, laid end to end along the dimension named above; an argument that names none is the same for every part.
All inputs are finite; a program needn't handle non-finite values.
Results may differ from the reference program's by a relative error of at most 0.012.
Values are sent between devices in bfloat16 or wider.
A program may use at most 2 GiB of HBM per device.

```python
import jax
import jax.numpy as jnp
from jax import lax

ROWS = 4096
D = 1024
HEADS = 32
KV_HEADS = 32
HEAD = 128
THETA = 10000


def setup_inputs(seed: int = 0, part: int = 0) -> dict:
    kx, kn, kq, kk, kv, ko = jax.random.split(jax.random.key(seed), 6)

    def weights(key, rows, columns):
        return jax.random.normal(key, (rows, columns), jnp.float32) * rows**-0.5

    drawn = {
        "x": jax.random.normal(jax.random.fold_in(kx, part), (ROWS, D), jnp.float32),
        "gain": 1 + 0.1 * jax.random.normal(kn, (D,), jnp.float32),
        "wq": 2 * weights(kq, D, HEADS * HEAD),
        "wk": 2 * weights(kk, D, KV_HEADS * HEAD),
        "wv": 4 * weights(kv, D, KV_HEADS * HEAD),
        "wo": weights(ko, HEADS * HEAD, D),
    }
    return {k: v.astype(jnp.bfloat16) for k, v in drawn.items()}


def normed(x, gain):
    wide = x.astype(jnp.float32)
    scale = lax.rsqrt(jnp.mean(wide * wide, -1, keepdims=True) + 1e-6)
    return (wide * scale * gain.astype(jnp.float32)).astype(jnp.bfloat16)


def turned(t, place, theta):
    half = t.shape[-1] // 2
    angle = place.astype(jnp.float32)[:, None] * theta ** (-jnp.arange(half, dtype=jnp.float32) / half)
    cos, sin = jnp.cos(angle)[:, None], jnp.sin(angle)[:, None]
    a, b = t[..., :half].astype(jnp.float32), t[..., half:].astype(jnp.float32)
    return jnp.concatenate([a * cos - b * sin, b * cos + a * sin], -1).astype(jnp.bfloat16)


def matmul(a, w):
    return jnp.dot(a, w, preferred_element_type=jnp.float32).astype(jnp.bfloat16)


def einsum(form, a, b):
    return jnp.einsum(form, a.astype(jnp.float32), b.astype(jnp.float32))


def attention(q, k, v):
    scores = einsum("tgsd,ugd->gstu", q, k) * q.shape[-1] ** -0.5
    token = jnp.arange(q.shape[0])
    scores = jnp.where(token[:, None] >= token, scores, -jnp.inf)
    weights = jax.nn.softmax(scores, -1).astype(jnp.bfloat16)
    return einsum("gstu,ugd->tgsd", weights, v).astype(jnp.bfloat16)


def reference(x, gain, wq, wk, wv, wo):
    a, place = normed(x, gain), jnp.arange(ROWS)
    q = turned(matmul(a, wq).reshape(ROWS, HEADS, HEAD), place, THETA).reshape(ROWS, KV_HEADS, -1, HEAD)
    k = turned(matmul(a, wk).reshape(ROWS, KV_HEADS, HEAD), place, THETA)
    v = matmul(a, wv).reshape(ROWS, KV_HEADS, HEAD)
    seen = attention(q, k, v).reshape(ROWS, HEADS * HEAD)
    return (x.astype(jnp.float32) + jnp.dot(seen, wo, preferred_element_type=jnp.float32)).astype(jnp.bfloat16)
```

```python
import functools

import jax
import jax.numpy as jnp
from jax import lax
from jax.experimental import pallas as pl
from jax.experimental.pallas import tpu as pltpu
from jax.sharding import PartitionSpec as P

HEAD = 128
THETA = 10000
NEG = -1e30
LOG2E = 1.4426950408889634
BF, F32 = jnp.bfloat16, jnp.float32

D = 1024
OWN = 1024
TOK = 4 * OWN
HEADS = 8
COLS = HEADS * HEAD
ROWS = D // 4
BLK = 512
HALF = BLK // 2
NB = TOK // BLK
PAIR = 2 * HEAD
PAIRS = COLS // PAIR
HR = ROWS // 2
E = HEAD**-0.5 * LOG2E


def _dot(a, b, ca, cb):
    return lax.dot_general(a, b, (((ca,), (cb,)), ((), ())), preferred_element_type=F32)


def _at(i, n):
    return pl.ds(i * n if isinstance(i, int) else pl.multiple_of(i * n, n), n)


def kernel(x_hbm, gain_ref, wq_hbm, wk_hbm, wv_hbm, wo_hbm, cos_ref, sin_ref, cosb_ref, sinb_ref, y_hbm,
           a_s, w_s, wo_s, q_s, k_s, v_s, p_s, accp_s, half_s, sendb_s, recvb_s, mix_s, top_s,
           loc_sem, locw_sem, pws, pwr, cws, cwr, fws, fwr, aps, apr, acs, acr, afs, afr, os_, or_, hs, hr, bs, br, y_sem):
    yy, s = lax.axis_index("dp"), lax.axis_index("sp")
    x, c = s // 2, s % 2
    ox = 1 - x
    partner, twin = (yy, 2 * x + 1 - c), (1 - yy, s)
    cross = lambda e: (yy, 2 * ox + e)
    ws = (wq_hbm, wk_hbm, wv_hbm)

    def remote(src, dst, ssem, rsem, dev):
        return pltpu.make_async_remote_copy(src_ref=src, dst_ref=dst, send_sem=ssem, recv_sem=rsem, device_id=dev,
                                            device_id_type=pl.DeviceIdType.MESH)

    load_x = pltpu.make_async_copy(x_hbm, a_s.at[_at(s, OWN)], loc_sem.at[0])
    load_wo = pltpu.make_async_copy(wo_hbm, wo_s, loc_sem.at[1])
    load_x.start()
    barrier = pltpu.get_barrier_semaphore()
    for dev in (partner, twin, cross(0), cross(1)):
        pl.semaphore_signal(barrier, inc=1, device_id=dev, device_id_type=pl.DeviceIdType.MESH)

    def col(t, g):
        return pl.ds(pl.multiple_of(t * COLS + g * PAIR, PAIR), PAIR)

    def w_local(g, m):
        return pltpu.make_async_copy(ws[m].at[:, col(s, g)], w_s.at[g, m, _at(s, ROWS)], locw_sem.at[g, m])

    def w_partner(g, m):
        return remote(ws[m].at[:, col(2 * x + 1 - c, g)], w_s.at[g, m, _at(s, ROWS)], pws.at[g, m], pwr.at[g, m], partner)

    def w_partner_in(g, m):
        here = w_s.at[g, m, _at(2 * x + 1 - c, ROWS)]
        return remote(here, here, pws.at[g, m], pwr.at[g, m], partner)

    def w_cross(g, m, e):
        rows = _at(yy, HR)
        return remote(ws[m].at[rows, col(2 * ox + e, g)], w_s.at[g, m, pl.ds(pl.multiple_of(s * ROWS + yy * HR, HR), HR)],
                      cws.at[g, m, e], cwr.at[g, m, c], cross(e))

    def w_cross_in(g, m, e):
        here = w_s.at[g, m, pl.ds(pl.multiple_of((2 * ox + e) * ROWS + yy * HR, HR), HR)]
        return remote(here, here, cws.at[g, m, e], cwr.at[g, m, e], cross(e))

    def w_twin(g, m, e):
        here = w_s.at[g, m, pl.ds(pl.multiple_of((2 * ox + e) * ROWS + yy * HR, HR), HR)]
        return remote(here, here, fws.at[g, m, e], fwr.at[g, m, e], twin)

    def w_twin_in(g, m, e):
        here = w_s.at[g, m, pl.ds(pl.multiple_of((2 * ox + e) * ROWS + (1 - yy) * HR, HR), HR)]
        return remote(here, here, fws.at[g, m, e], fwr.at[g, m, e], twin)

    pl.semaphore_wait(barrier, 4)
    for g in range(PAIRS):
        for e in range(2):
            for m in range(3):
                w_cross(g, m, e).start()
        for m in range(3):
            w_partner(g, m).start()
            w_local(g, m).start()
    load_wo.start()

    load_x.wait()

    def norm(i, _):
        rows = pl.ds(pl.multiple_of(s * OWN + i * 128, 128), 128)
        wide = a_s[rows, :].astype(F32)
        scale = lax.rsqrt(jnp.mean(wide * wide, -1, keepdims=True) + 1e-6)
        a_s[rows, :] = (wide * scale * gain_ref[...].astype(F32)).astype(BF)

    lax.fori_loop(0, OWN // 128, norm, None)

    def a_partner(j):
        here = a_s.at[_at(2 * s + j, BLK)]
        return remote(here, here, aps.at[j], apr.at[j], partner)

    def a_partner_in(j):
        here = a_s.at[_at(2 * (2 * x + 1 - c) + j, BLK)]
        return remote(here, here, aps.at[j], apr.at[j], partner)

    def a_cross(j):
        here = a_s.at[_at((4 * x + j) * 2 + c, HALF)]
        return remote(here, here, acs.at[j], acr.at[j], cross(c))

    def a_cross_in(j):
        here = a_s.at[_at((4 * ox + j) * 2 + c, HALF)]
        return remote(here, here, acs.at[j], acr.at[j], cross(c))

    def a_hand(j):
        here = a_s.at[_at((4 * ox + j) * 2 + c, HALF)]
        return remote(here, here, afs.at[j], afr.at[j], partner)

    def a_hand_in(j):
        here = a_s.at[_at((4 * ox + j) * 2 + 1 - c, HALF)]
        return remote(here, here, afs.at[j], afr.at[j], partner)

    def project(r, n, g):
        r = pl.multiple_of(r, n)
        a = a_s[pl.ds(r, n), :]
        b = r // BLK
        inner = pl.ds(pl.multiple_of(r % BLK, n), n)
        cr, sr = cos_ref[inner, :], sin_ref[inner, :]
        cb, sb = cosb_ref[pl.ds(b, 1), :], sinb_ref[pl.ds(b, 1), :]
        cos = cb * cr - sb * sr
        sin = sb * cr + cb * sr
        sin = jnp.where(lax.broadcasted_iota(jnp.int32, sin.shape, 1) < HEAD // 2, -sin, sin)
        own = b // 4 == x
        rq = pl.multiple_of(jnp.where(own, r - 4 * x * BLK, 4 * BLK + r % BLK), n)

        def turned(t):
            t = t.astype(BF).astype(F32)
            return (t * cos + pltpu.roll(t, HEAD // 2, 1) * sin).astype(BF)

        q, k, v = (_dot(a, w_s[g, m], 1, 0) for m in range(3))
        for h in range(2):
            cut = slice(h * HEAD, (h + 1) * HEAD)
            q_s[2 * g + h, pl.ds(rq, n), :] = turned(q[:, cut])
            k_s[2 * g + h, pl.ds(r, n), :] = turned(k[:, cut])
            v_s[2 * g + h, :, pl.ds(r, n)] = v[:, cut].T.astype(BF)

    def take(g):
        for m in range(3):
            w_local(g, m).wait()
            w_partner_in(g, m).wait_recv()
            for e in range(2):
                w_twin_in(g, m, e).wait_recv()
        lax.fori_loop(0, 4, lambda j, _: project((4 * x + j) * BLK, BLK, g), None)

    def arrive(g):
        for e in range(2):
            for m in range(3):
                w_cross_in(g, m, e).wait_recv()
                w_twin(g, m, e).start()

    def weights(g, _):
        arrive(g)

        @pl.when(g == 1)
        def _():
            for j in range(2):
                a_partner(j).start()

        @pl.when(g == 2)
        def _():
            for j in range(2):
                a_partner_in(j).wait_recv()
            for j in range(4):
                a_cross(j).start()

        @pl.when(g >= 2)
        def _():
            take(g - 2)

    lax.fori_loop(0, PAIRS, weights, None)
    lax.fori_loop(PAIRS - 2, PAIRS, lambda g, _: take(g), None)
    load_wo.wait()

    ones = jnp.ones((8, BLK), BF)
    hidden = lax.broadcasted_iota(jnp.int32, (HALF, HALF), 0) > lax.broadcasted_iota(jnp.int32, (HALF, HALF), 1)

    def place(b):
        return pl.multiple_of(jnp.where(b // 4 == x, (b - 4 * x) * BLK, 4 * BLK), BLK)

    def attend(b):
        at_q = place(b)
        top_s[...] = jnp.full(top_s.shape, NEG, F32)
        mix_s[...] = jnp.zeros(mix_s.shape, F32)
        pieces = [(h, i) for h in range(HEADS) for i in range(2)]

        def step(j, diagonal):
            first = j * BLK
            scores = []
            for h, i in pieces:
                n = HALF if diagonal and i == 0 else BLK
                keys = k_s[h, pl.ds(pl.multiple_of(first, BLK), n), :]
                scores.append(_dot(keys, q_s[h, pl.ds(pl.multiple_of(at_q + i * HALF, HALF), HALF), :], 1, 1))
            weights, keeps = [], []
            for (h, i), t in zip(pieces, scores):
                if diagonal:
                    cut = jnp.where(hidden, 2 * NEG, t[-HALF:, :])
                    t = cut if i == 0 else jnp.concatenate([t[:HALF, :], cut], axis=0)
                old = top_s[2 * h + i : 2 * h + i + 1, :]
                top = jnp.maximum(old, t.max(axis=0, keepdims=True))
                top_s[2 * h + i : 2 * h + i + 1, :] = top
                weights.append(jnp.exp2((t - top) * E).astype(BF))
                keeps.append(jnp.exp2((old - top) * E))
            for (h, i), p, keep in zip(pieces, weights, keeps):
                n = p.shape[0]
                values = jnp.concatenate([v_s[h, :, pl.ds(pl.multiple_of(first, BLK), n)], ones[:, :n]], axis=0)
                mix_s[h, i] = mix_s[h, i] * keep + _dot(values, p, 1, 0)

        lax.fori_loop(0, b, lambda j, _: step(j, False), None)
        step(b, True)
        for h, i in pieces:
            total = mix_s[h, i, HEAD : HEAD + 1, :]
            q_s[h, pl.ds(pl.multiple_of(at_q + i * HALF, HALF), HALF), :] = (mix_s[h, i, :HEAD, :] * (1 / total)).T.astype(BF)

    def output(b):
        seen = jnp.concatenate([q_s[h, pl.ds(place(b), BLK), :] for h in range(HEADS)], axis=1)

        def tile(n, _):
            p_s[:, _at(n, PAIR)] = _dot(seen, wo_s[:, _at(n, PAIR)], 1, 0)

        lax.fori_loop(0, D // PAIR, tile, None)

    def to_owner(b):
        return remote(p_s, accp_s.at[b % 2], os_.at[b % 2], or_.at[b % 2], partner)

    def to_half(b):
        return remote(p_s.at[_at(1 - c, HALF)], half_s.at[b % 2], hs.at[b % 2], hr.at[b % 2], partner)

    def to_cross(b):
        return remote(sendb_s.at[b % 2], recvb_s.at[b % 2, _at(c, HALF)], bs.at[b % 2], br.at[b % 2, c], (yy, b // 2))

    def send(b):
        @pl.when((b // 4 == x) & (b // 2 != s))
        def _():
            to_owner(b).start()

        @pl.when(b // 4 != x)
        def _():
            to_half(b).start()

    def finish(b):
        @pl.when(b // 2 == s)
        def _():
            to_owner(b).wait_recv()

            def add(i, _):
                rows = _at(i, 64)
                accp_s[b % 2, rows, :] += p_s[rows, :]

            lax.fori_loop(0, BLK // 64, add, None)

        @pl.when((b // 4 == x) & (b // 2 != s))
        def _():
            to_owner(b).wait_send()

        @pl.when(b // 4 != x)
        def _():
            to_half(b).wait_send()
            to_half(b).wait_recv()

            @pl.when(b % 4 >= 2)
            def _():
                to_cross(b - 2).wait_send()

            def add(i, _):
                rows = pl.ds(pl.multiple_of(c * HALF + i * 64, 64), 64)
                sendb_s[b % 2, _at(i, 64), :] = (p_s[rows, :] + half_s[b % 2, _at(i, 64), :]).astype(BF)

            lax.fori_loop(0, HALF // 64, add, None)
            to_cross(b).start()

    def block(b, _):
        @pl.when(b // 4 != x)
        def _():
            j = b - 4 * ox
            a_cross_in(j).wait_recv()
            a_hand(j).start()
            lax.fori_loop(0, PAIRS, lambda g, _: project(b * BLK + c * HALF, HALF, g), None)
            a_hand_in(j).wait_recv()
            lax.fori_loop(0, PAIRS, lambda g, _: project(b * BLK + (1 - c) * HALF, HALF, g), None)

        attend(b)

        @pl.when(b > 0)
        def _():
            finish(b - 1)

        output(b)
        send(b)

    lax.fori_loop(0, NB, block, None)
    finish(NB - 1)

    for j in range(2):
        a_partner(j).wait_send()
    for j in range(4):
        a_cross(j).wait_send()
        a_hand(j).wait_send()
    load_x.start()
    for g in range(PAIRS):
        for m in range(3):
            w_partner(g, m).wait_send()
            for e in range(2):
                w_cross(g, m, e).wait_send()
                w_twin(g, m, e).wait_send()
    load_x.wait()

    for n in range(2):
        for e in range(2):
            here = recvb_s.at[n, _at(e, HALF)]
            remote(here, here, bs.at[n], br.at[n, e], cross(e)).wait_recv()

        def add(i, _):
            rows = _at(i, 64)
            old = a_s[pl.ds(pl.multiple_of(s * OWN + n * BLK + i * 64, 64), 64), :].astype(F32)
            recvb_s[n, rows, :] = (old + (accp_s[n, rows, :] + recvb_s[n, rows, :].astype(F32))).astype(BF)

        lax.fori_loop(0, BLK // 64, add, None)
        pltpu.make_async_copy(recvb_s.at[n], y_hbm.at[_at(n, BLK)], y_sem.at[n]).start()
    for n in range(2):
        pltpu.make_async_copy(recvb_s.at[n], y_hbm.at[_at(n, BLK)], y_sem.at[n]).wait()
    for j in range(2, 4):
        to_cross(4 * ox + j).wait_send()


def solution(mesh):
    def tables(at):
        half = HEAD // 2
        angle = at.astype(F32)[:, None] * THETA ** (-jnp.arange(half, dtype=F32) / half)
        return (jnp.concatenate([t, t], -1) for t in (jnp.cos(angle), jnp.sin(angle)))

    def step(x, gain, wq, wk, wv, wo):
        cos, sin = tables(jnp.arange(BLK))
        cosb, sinb = tables(jnp.arange(NB) * BLK)
        hbm, vmem = pl.BlockSpec(memory_space=pl.ANY), pl.BlockSpec(memory_space=pltpu.VMEM)
        dma = pltpu.SemaphoreType.DMA
        return pl.pallas_call(
            kernel,
            out_shape=jax.ShapeDtypeStruct((OWN, D), BF),
            in_specs=[hbm, vmem, hbm, hbm, hbm, hbm, vmem, vmem, vmem, vmem],
            out_specs=hbm,
            scratch_shapes=[
                pltpu.VMEM((TOK, D), BF),
                pltpu.VMEM((PAIRS, 3, D, PAIR), BF),
                pltpu.VMEM((COLS, D), BF),
                pltpu.VMEM((HEADS, 5 * BLK, HEAD), BF),
                pltpu.VMEM((HEADS, TOK, HEAD), BF),
                pltpu.VMEM((HEADS, HEAD, TOK), BF),
                pltpu.VMEM((BLK, D), F32),
                pltpu.VMEM((2, BLK, D), F32),
                pltpu.VMEM((2, HALF, D), F32),
                pltpu.VMEM((2, HALF, D), BF),
                pltpu.VMEM((2, BLK, D), BF),
                pltpu.VMEM((HEADS, 2, HEAD + 8, HALF), F32),
                pltpu.VMEM((2 * HEADS, HALF), F32),
                dma((2,)), dma((PAIRS, 3)),
                dma((PAIRS, 3)), dma((PAIRS, 3)),
                dma((PAIRS, 3, 2)), dma((PAIRS, 3, 2)),
                dma((PAIRS, 3, 2)), dma((PAIRS, 3, 2)),
                dma((2,)), dma((2,)),
                dma((4,)), dma((4,)), dma((4,)), dma((4,)),
                dma((2,)), dma((2,)), dma((2,)), dma((2,)),
                dma((2,)), dma((2, 2)), dma((2,)),
            ],
            compiler_params=pltpu.CompilerParams(collective_id=0, has_side_effects=True, vmem_limit_bytes=67043328),
        )(x, gain.reshape(1, D), wq, wk, wv, wo, cos, sin, cosb, sinb)

    tokens, whole = P(("dp", "sp"), None), P("sp", None)
    return jax.shard_map(
        step,
        mesh=mesh,
        in_specs=(tokens, P(None), whole, whole, whole, whole),
        out_specs=tokens,
        check_vma=False,
    )
```

```python
import jax
import jax.numpy as jnp
import numpy as np
from jax import lax
from jax.experimental import pallas as pl
from jax.experimental.pallas import tpu as pltpu
from jax.sharding import PartitionSpec as P

HEAD = 128
THETA = 10000
NEG = -1e30
LOG2E = 1.4426950408889634
BF, F32 = jnp.bfloat16, jnp.float32

D = 1024
OWN = 1024
TOK = 4 * OWN
HEADS = 8
COLS = HEADS * HEAD
ROWS = D // 4
BLK = 512
HALF = BLK // 2
NB = TOK // BLK
PAIR = 2 * HEAD
PAIRS = COLS // PAIR
HR = ROWS // 2
E = HEAD**-0.5 * LOG2E
NEAR, DIAG, WHOLE = (3, 1), (3, 1), (1, 1)


def _dot(a, b, ca, cb):
    return lax.dot_general(a, b, (((ca,), (cb,)), ((), ())), preferred_element_type=F32)


def _at(i, n):
    return pl.ds(i * n if isinstance(i, int) else pl.multiple_of(i * n, n), n)


def kernel(x_hbm, gain_ref, wq_hbm, wk_hbm, wv_hbm, wo_hbm, cos_ref, sin_ref, cosb_ref, sinb_ref, y_hbm,
           st_hbm, a_s, w_s, wo_s, q_s, k_s, v_s, p_s, accp_s, sendb_s, recvb_s, mix_s, top_s, top1_s,
           loc_sem, st_sem, locw_sem, pws, pwr, cws, cwr, fws, fwr, aps, apr, acs, acr, afs, afr, os_, or_, hs, hr, bs, br, y_sem):
    yy, s = lax.axis_index("dp"), lax.axis_index("sp")
    x, c = s // 2, s % 2
    ox = 1 - x
    partner, twin = (yy, 2 * x + 1 - c), (1 - yy, s)
    cross = lambda e: (yy, 2 * ox + e)
    ws = (wq_hbm, wk_hbm, wv_hbm)

    def remote(src, dst, ssem, rsem, dev):
        return pltpu.make_async_remote_copy(src_ref=src, dst_ref=dst, send_sem=ssem, recv_sem=rsem, device_id=dev,
                                            device_id_type=pl.DeviceIdType.MESH)

    load_x = pltpu.make_async_copy(x_hbm, a_s.at[_at(s, OWN)], loc_sem.at[0])
    load_wo = pltpu.make_async_copy(wo_hbm, wo_s, loc_sem.at[1])
    load_x.start()
    barrier = pltpu.get_barrier_semaphore()
    for dev in (partner, twin, cross(0), cross(1)):
        pl.semaphore_signal(barrier, inc=1, device_id=dev, device_id_type=pl.DeviceIdType.MESH)

    def col(t, g):
        return pl.ds(pl.multiple_of(t * COLS + g * PAIR, PAIR), PAIR)

    def w_local(g, m):
        return pltpu.make_async_copy(ws[m].at[:, col(s, g)], w_s.at[g, m, _at(s, ROWS)], locw_sem.at[g, m])

    def w_partner(g, m):
        return remote(ws[m].at[:, col(2 * x + 1 - c, g)], w_s.at[g, m, _at(s, ROWS)], pws.at[g, m], pwr.at[g, m], partner)

    def w_partner_in(g, m):
        here = w_s.at[g, m, _at(2 * x + 1 - c, ROWS)]
        return remote(here, here, pws.at[g, m], pwr.at[g, m], partner)

    def w_cross(g, m, e):
        rows = _at(yy, HR)
        return remote(ws[m].at[rows, col(2 * ox + e, g)], w_s.at[g, m, pl.ds(pl.multiple_of(s * ROWS + yy * HR, HR), HR)],
                      cws.at[g, m, e], cwr.at[g, m, c], cross(e))

    def w_cross_in(g, m, e):
        here = w_s.at[g, m, pl.ds(pl.multiple_of((2 * ox + e) * ROWS + yy * HR, HR), HR)]
        return remote(here, here, cws.at[g, m, e], cwr.at[g, m, e], cross(e))

    def w_twin(g, m, e):
        here = w_s.at[g, m, pl.ds(pl.multiple_of((2 * ox + e) * ROWS + yy * HR, HR), HR)]
        return remote(here, here, fws.at[g, m, e], fwr.at[g, m, e], twin)

    def w_twin_in(g, m, e):
        here = w_s.at[g, m, pl.ds(pl.multiple_of((2 * ox + e) * ROWS + (1 - yy) * HR, HR), HR)]
        return remote(here, here, fws.at[g, m, e], fwr.at[g, m, e], twin)

    pl.semaphore_wait(barrier, 4)
    for g in range(PAIRS):
        for m in range(3):
            for e in range(2):
                w_cross(g, m, e).start()
        for m in range(3):
            w_partner(g, m).start()
            w_local(g, m).start()
    load_wo.start()

    load_x.wait()

    gain = gain_ref[...].astype(F32).reshape(1, D)

    def norm(i, _):
        rows = pl.ds(pl.multiple_of(s * OWN + i * 128, 128), 128)
        wide = a_s[rows, :].astype(F32)
        scale = lax.rsqrt(jnp.mean(wide * wide, -1, keepdims=True) + 1e-6)
        a_s[rows, :] = (wide * scale * gain).astype(BF)

    lax.fori_loop(0, OWN // 128, norm, None)

    def a_partner(j):
        here = a_s.at[_at(2 * s + j, BLK)]
        return remote(here, here, aps.at[j], apr.at[j], partner)

    def a_partner_in(j):
        here = a_s.at[_at(2 * (2 * x + 1 - c) + j, BLK)]
        return remote(here, here, aps.at[j], apr.at[j], partner)

    def a_cross(j):
        here = a_s.at[_at((4 * x + j) * 2 + c, HALF)]
        return remote(here, here, acs.at[j], acr.at[j], cross(c))

    def a_cross_in(j):
        here = a_s.at[_at((4 * ox + j) * 2 + c, HALF)]
        return remote(here, here, acs.at[j], acr.at[j], cross(c))

    def a_hand(j):
        here = a_s.at[_at((4 * ox + j) * 2 + c, HALF)]
        return remote(here, here, afs.at[j], afr.at[j], partner)

    def a_hand_in(j):
        here = a_s.at[_at((4 * ox + j) * 2 + 1 - c, HALF)]
        return remote(here, here, afs.at[j], afr.at[j], partner)

    def place(b):
        return pl.multiple_of(jnp.where(b // 4 == x, (b - 4 * x) * BLK, 4 * BLK), BLK)

    def project(b, g):
        rows, at_q = _at(b, BLK), pl.ds(place(b), BLK)
        a = a_s[rows, :]
        cr, sr = cos_ref[...], sin_ref[...]
        cb, sb = cosb_ref[pl.ds(b, 1), :], sinb_ref[pl.ds(b, 1), :]
        cos = cb * cr - sb * sr
        sin = sb * cr + cb * sr
        sin = jnp.where(lax.broadcasted_iota(jnp.int32, sin.shape, 1) < HEAD // 2, -sin, sin)

        def turned(t):
            t = t.astype(BF).astype(F32)
            return (t * cos + pltpu.roll(t, HEAD // 2, 1) * sin).astype(BF)

        q, k, v = (_dot(a, w_s[g, m], 1, 0) for m in range(3))
        for h in range(2):
            cut = slice(h * HEAD, (h + 1) * HEAD)
            q_s[2 * g + h, at_q, :] = turned(q[:, cut])
            k_s[2 * g + h, rows, :] = turned(k[:, cut])
            v_s[2 * g + h, :, rows] = v[:, cut].T.astype(BF)

    hidden = lax.broadcasted_iota(jnp.int32, (HALF, HALF), 0) > lax.broadcasted_iota(jnp.int32, (HALF, HALF), 1)

    def pieces(todo, ahead, lag):
        scores, weights = {}, {}
        for t in range(len(todo) + ahead + lag):
            if t < len(todo):
                h, at, n, first, keys, _ = todo[t][0]
                scores[t] = _dot(k_s[h, pl.ds(first, keys), :], q_s[h, pl.ds(at, n), :], 1, 1)
            if 0 <= t - ahead < len(todo):
                (h, at, n, first, keys, masked), (m, row, lanes), old = todo[t - ahead]
                e = scores.pop(t - ahead)
                if masked:
                    cut = jnp.where(hidden, 2 * NEG, e[-HALF:, :])
                    e = cut if keys == HALF else jnp.concatenate([e[:-HALF, :], cut], axis=0)
                top = e.max(axis=0, keepdims=True)
                keep = None
                if old:
                    before = row[:, lanes]
                    top = jnp.maximum(before, top)
                    keep = jnp.exp2((before - top) * E)
                row[:, lanes] = top
                weights[t - ahead] = jnp.exp2((e - top) * E).astype(BF), keep
            if 0 <= t - ahead - lag:
                (h, at, n, first, keys, masked), (m, row, lanes), old = todo[t - ahead - lag]
                p, keep = weights.pop(t - ahead - lag)
                got = _dot(jnp.concatenate([v_s[h, :, pl.ds(first, keys)], jnp.ones((8, keys), BF)], axis=0), p, 1, 0)
                mix_s[m, :, lanes] = mix_s[m, :, lanes] * keep + got if old else got

    def cut(i):
        return slice(i * HALF, (i + 1) * HALF)

    def state_out(g):
        return pltpu.make_async_copy(mix_s, st_hbm.at[g], st_sem.at[g])

    def state_in(j, g):
        return pltpu.make_async_copy(st_hbm.at[g, _at(j, 2)], mix_s.at[pl.ds(2 * g, 2)], st_sem.at[g])

    def near(g):
        todo = []
        for j in range(4):
            for h in range(2):
                for i in range(2):
                    piece = 2 * g + h, j * BLK + i * HALF, HALF, pl.multiple_of(4 * x * BLK, BLK), j * BLK + (i + 1) * HALF, True
                    todo.append((piece, (2 * j + h, top1_s.at[j, pl.ds(2 * g + h, 1)], cut(i)), False))
        pieces(todo, *NEAR)
        state_out(g).start()

    def diagonal(b, lead):
        todo = []
        for h in range(HEADS):
            for i in range(2):
                first = pl.multiple_of((b - lead) * BLK, BLK)
                piece = h, 4 * BLK + i * HALF, HALF, first, lead * BLK + (i + 1) * HALF, True
                todo.append((piece, (h, top_s.at[h : h + 1], cut(i)), False))
        pieces(todo, *DIAG)

    def whole(at_q, j):
        first = pl.multiple_of(2 * j * BLK, 2 * BLK)
        pieces([((h, at_q, BLK, first, 2 * BLK, False), (h, top_s.at[h : h + 1], slice(0, BLK)), True) for h in range(HEADS)], *WHOLE)

    def attend(at_q, steps):
        lax.fori_loop(0, steps, lambda j, _: whole(at_q, j), None)
        for h in range(HEADS):
            got = mix_s[h, :HEAD, :] * (1 / mix_s[h, HEAD : HEAD + 1, :])
            q_s[h, pl.ds(at_q, BLK), :] = got.T.astype(BF)

    def output(at_q, slot):
        seen = jnp.concatenate([q_s[h, pl.ds(at_q, BLK), :] for h in range(HEADS)], axis=1)
        for n in range(0, D, PAIR):
            p_s[slot, :, n : n + PAIR] = _dot(seen, wo_s[:, n : n + PAIR], 1, 0)

    def hand(j):
        a_cross_in(j).wait_recv()
        a_hand(j).start()

    def arrive(g, m):
        for e in range(2):
            w_cross_in(g, m, e).wait_recv()
            w_twin(g, m, e).start()

    def near_weights(g):
        for m in range(3):
            w_local(g, m).wait()
            w_partner_in(g, m).wait_recv()

    def twin_weights(g):
        for m in range(3):
            for e in range(2):
                w_twin_in(g, m, e).wait_recv()

    def take(dev, g):
        for j in range(2):
            project(2 * dev + j, g)

    near_weights(0)
    for j in range(2):
        a_partner(j).start()
    for m in range(3):
        arrive(0, m)

    def weights(g, _):
        @pl.when(g > 0)
        def _():
            near_weights(g)

        twin_weights(g)

        def rows(i, _):
            @pl.when(g < PAIRS - 1)
            def _():
                for m in range(2):
                    @pl.when(i == m)
                    def _():
                        arrive(g + 1, m)

            @pl.when((g == 0) & (i == 1))
            def _():
                for j in range(2):
                    a_partner_in(j).wait_recv()

            take(jnp.where(i == 0, s, 2 * x + 1 - c), g)

        lax.fori_loop(0, 2, rows, None)

        @pl.when(g < PAIRS - 1)
        def _():
            arrive(g + 1, 2)

        @pl.when((g == 1) | (g == 2))
        def _():
            for j in range(2):
                a_cross(2 * (g - 1) + j).start()

        @pl.when(g == PAIRS - 1)
        def _():
            hand(0)

        @pl.when(g > 0)
        def _():
            state_out(g - 1).wait()

        near(g)

    lax.fori_loop(0, PAIRS, weights, None)
    load_wo.wait()

    def turn(t):
        return t % 2 * 2 + t // 2

    def to_owner(b, t):
        return remote(p_s.at[t % 2], accp_s.at[b % 2], os_.at[b % 2], or_.at[b % 2], partner)

    def to_half(b):
        return remote(p_s.at[0, _at(1 - c, HALF)], p_s.at[1, _at(b % 2, HALF)], hs.at[b % 2], hr.at[b % 2], partner)

    def to_cross(b):
        return remote(sendb_s.at[b % 2], recvb_s.at[b % 2, _at(c, HALF)], bs.at[b % 2], br.at[b % 2, c], (yy, b // 2))

    def finish_far(j):
        b = 4 * ox + j
        to_half(b).wait_send()
        to_half(b).wait_recv()

        @pl.when(j >= 2)
        def _():
            to_cross(b - 2).wait_send()

        def add(i, _):
            rows = pl.ds(pl.multiple_of(c * HALF + i * 64, 64), 64)
            sendb_s[b % 2, _at(i, 64), :] = (p_s[0, rows, :] + p_s[1, pl.ds(pl.multiple_of(b % 2 * HALF + i * 64, 64), 64), :]).astype(BF)

        lax.fori_loop(0, HALF // 64, add, None)
        to_cross(b).start()

    def y_out(n):
        return pltpu.make_async_copy(recvb_s.at[n], y_hbm.at[_at(n, BLK)], y_sem.at[n])

    def finish_own(t):
        b = 4 * x + turn(t)
        n = b % 2

        @pl.when(b // 2 == s)
        def _():
            for e in range(2):
                here = recvb_s.at[n, _at(e, HALF)]
                remote(here, here, bs.at[n], br.at[n, e], cross(e)).wait_recv()
            to_owner(b, t).wait_recv()

            def add(i, _):
                rows = _at(i, 64)
                total = p_s[t % 2, rows, :] + accp_s[n, rows, :] + recvb_s[n, rows, :].astype(F32)
                old = a_s[pl.ds(pl.multiple_of(b * BLK + i * 64, 64), 64), :].astype(F32)
                recvb_s[n, rows, :] = (old + total).astype(BF)

            lax.fori_loop(0, BLK // 64, add, None)
            y_out(n).start()

        @pl.when(b // 2 != s)
        def _():
            to_owner(b, t).wait_send()

    state_out(PAIRS - 1).wait()

    def far(j, _):
        b = 4 * ox + j
        a_hand_in(j).wait_recv()

        def both(i, _):
            project(b, 2 * i)
            project(b, 2 * i + 1)

        lax.fori_loop(0, PAIRS // 2, both, None)

        @pl.when(j > 0)
        def _():
            finish_far(j - 1)

        @pl.when(b % 2 == 0)
        def _():
            diagonal(b, 0)

        @pl.when(b % 2 == 1)
        def _():
            diagonal(b, 1)

        attend(4 * BLK, b // 2)

        @pl.when(j < 3)
        def _():
            hand(j + 1)

        @pl.when(j == 3)
        def _():
            for g in range(PAIRS):
                state_in(0, g).start()

        output(4 * BLK, 0)
        to_half(b).start()

    lax.fori_loop(0, 4, far, None)

    def own(t, _):
        j = turn(t)
        b = 4 * x + j
        for g in range(PAIRS):
            state_in(j, g).wait()
        top_s[...] = top1_s[j]
        at_q = pl.multiple_of(j * BLK, BLK)
        attend(at_q, 2 * x)

        @pl.when(t < 3)
        def _():
            for g in range(PAIRS):
                state_in(turn(t + 1), g).start()

        @pl.when(t == 0)
        def _():
            finish_far(3)

        output(at_q, t % 2)

        @pl.when(b // 2 != s)
        def _():
            to_owner(b, t).start()

        @pl.when(t == 1)
        def _():
            load_x.wait()

        @pl.when(t > 0)
        def _():
            finish_own(t - 1)

    for j in range(2):
        a_partner(j).wait_send()
    for j in range(4):
        a_cross(j).wait_send()
        a_hand(j).wait_send()
    load_x.start()
    for g in range(PAIRS):
        for m in range(3):
            w_partner(g, m).wait_send()
            for e in range(2):
                w_cross(g, m, e).wait_send()
                w_twin(g, m, e).wait_send()
    lax.fori_loop(0, 4, own, None)
    finish_own(3)
    for n in range(2):
        y_out(n).wait()
    for j in range(2, 4):
        to_cross(4 * ox + j).wait_send()


def tables(at):
    half = HEAD // 2
    angle = at[:, None] * float(THETA) ** (-np.arange(half) / half)
    return (np.concatenate([t, t], -1).astype(np.float32) for t in (np.cos(angle), np.sin(angle)))


def solution(mesh):
    def step(x, gain, wq, wk, wv, wo):
        cos, sin = tables(np.arange(BLK))
        cosb, sinb = tables(np.arange(NB) * BLK)
        hbm, vmem = pl.BlockSpec(memory_space=pl.ANY), pl.BlockSpec(memory_space=pltpu.VMEM)
        dma = pltpu.SemaphoreType.DMA
        return pl.pallas_call(
            kernel,
            out_shape=[jax.ShapeDtypeStruct((OWN, D), BF), jax.ShapeDtypeStruct((PAIRS, HEADS, HEAD + 8, BLK), F32)],
            in_specs=[hbm, vmem, hbm, hbm, hbm, hbm, vmem, vmem, vmem, vmem],
            out_specs=[hbm, hbm],
            scratch_shapes=[
                pltpu.VMEM((TOK, D), BF),
                pltpu.VMEM((PAIRS, 3, D, PAIR), BF),
                pltpu.VMEM((COLS, D), BF),
                pltpu.VMEM((HEADS, 5 * BLK, HEAD), BF),
                pltpu.VMEM((HEADS, TOK, HEAD), BF),
                pltpu.VMEM((HEADS, HEAD, TOK), BF),
                pltpu.VMEM((2, BLK, D), F32),
                pltpu.VMEM((2, BLK, D), F32),
                pltpu.VMEM((2, HALF, D), BF),
                pltpu.VMEM((2, BLK, D), BF),
                pltpu.VMEM((HEADS, HEAD + 8, BLK), F32),
                pltpu.VMEM((HEADS, BLK), F32),
                pltpu.VMEM((4, HEADS, BLK), F32),
                dma((2,)), dma((PAIRS,)), dma((PAIRS, 3)),
                dma((PAIRS, 3)), dma((PAIRS, 3)),
                dma((PAIRS, 3, 2)), dma((PAIRS, 3, 2)),
                dma((PAIRS, 3, 2)), dma((PAIRS, 3, 2)),
                dma((2,)), dma((2,)),
                dma((4,)), dma((4,)), dma((4,)), dma((4,)),
                dma((2,)), dma((2,)), dma((2,)), dma((2,)),
                dma((2,)), dma((2, 2)), dma((2,)),
            ],
            compiler_params=pltpu.CompilerParams(collective_id=0, has_side_effects=True, vmem_limit_bytes=67043328),
        )(x, gain, wq, wk, wv, wo, cos, sin, cosb, sinb)[0]

    tokens, whole = P(("dp", "sp"), None), P("sp", None)
    return jax.shard_map(
        step,
        mesh=mesh,
        in_specs=(tokens, P(None), whole, whole, whole, whole),
        out_specs=tokens,
        check_vma=False,
    )
```

```python
import jax
import jax.numpy as jnp
import numpy as np
from jax import lax
from jax.experimental import pallas as pl
from jax.experimental.pallas import tpu as pltpu
from jax.sharding import PartitionSpec as P

HEAD = 128
THETA = 10000
NEG = -1e30
LOG2E = 1.4426950408889634
BF, F32 = jnp.bfloat16, jnp.float32

D = 1024
OWN = 1024
TOK = 4 * OWN
HEADS = 8
COLS = HEADS * HEAD
ROWS = D // 4
BLK = 512
HALF = BLK // 2
NB = TOK // BLK
PAIR = 2 * HEAD
PAIRS = COLS // PAIR
HR = ROWS // 2
E = HEAD**-0.5 * LOG2E
NEAR, DIAG, WHOLE = (3, 1), (3, 1), (1, 1)


def _dot(a, b, ca, cb):
    return lax.dot_general(a, b, (((ca,), (cb,)), ((), ())), preferred_element_type=F32)


def _at(i, n):
    return pl.ds(i * n if isinstance(i, int) else pl.multiple_of(i * n, n), n)


def kernel(x_hbm, gain_ref, wq_hbm, wk_hbm, wv_hbm, wo_hbm, cos_ref, sin_ref, cosb_ref, sinb_ref, y_hbm,
           st_hbm, a_s, w_s, wo_s, q_s, k_s, v_s, p_s, accp_s, sendb_s, recvb_s, mix_s, top_s, top1_s,
           loc_sem, st_sem, locw_sem, pws, pwr, cws, cwr, fws, fwr, aps, apr, acs, acr, afs, afr, os_, or_, hs, hr, bs, br, y_sem):
    yy, s = lax.axis_index("dp"), lax.axis_index("sp")
    x, c = s // 2, s % 2
    ox = 1 - x
    partner, twin = (yy, 2 * x + 1 - c), (1 - yy, s)
    cross = lambda e: (yy, 2 * ox + e)
    ws = (wq_hbm, wk_hbm, wv_hbm)

    def remote(src, dst, ssem, rsem, dev):
        return pltpu.make_async_remote_copy(src_ref=src, dst_ref=dst, send_sem=ssem, recv_sem=rsem, device_id=dev,
                                            device_id_type=pl.DeviceIdType.MESH)

    load_x = pltpu.make_async_copy(x_hbm, a_s.at[_at(s, OWN)], loc_sem.at[0])
    load_wo = pltpu.make_async_copy(wo_hbm, wo_s, loc_sem.at[1])
    load_x.start()
    barrier = pltpu.get_barrier_semaphore()
    for dev in (partner, twin, cross(0), cross(1)):
        pl.semaphore_signal(barrier, inc=1, device_id=dev, device_id_type=pl.DeviceIdType.MESH)

    def col(t, g):
        return pl.ds(pl.multiple_of(t * COLS + g * PAIR, PAIR), PAIR)

    def w_local(g, m):
        return pltpu.make_async_copy(ws[m].at[:, col(s, g)], w_s.at[g, m, _at(s, ROWS)], locw_sem.at[g, m])

    def w_partner(g, m):
        return remote(ws[m].at[:, col(2 * x + 1 - c, g)], w_s.at[g, m, _at(s, ROWS)], pws.at[g, m], pwr.at[g, m], partner)

    def w_partner_in(g, m):
        here = w_s.at[g, m, _at(2 * x + 1 - c, ROWS)]
        return remote(here, here, pws.at[g, m], pwr.at[g, m], partner)

    def w_cross(g, m, e):
        rows = _at(yy, HR)
        return remote(ws[m].at[rows, col(2 * ox + e, g)], w_s.at[g, m, pl.ds(pl.multiple_of(s * ROWS + yy * HR, HR), HR)],
                      cws.at[g, m, e], cwr.at[g, m, c], cross(e))

    def w_cross_in(g, m, e):
        here = w_s.at[g, m, pl.ds(pl.multiple_of((2 * ox + e) * ROWS + yy * HR, HR), HR)]
        return remote(here, here, cws.at[g, m, e], cwr.at[g, m, e], cross(e))

    def w_twin(g, m, e):
        here = w_s.at[g, m, pl.ds(pl.multiple_of((2 * ox + e) * ROWS + yy * HR, HR), HR)]
        return remote(here, here, fws.at[g, m, e], fwr.at[g, m, e], twin)

    def w_twin_in(g, m, e):
        here = w_s.at[g, m, pl.ds(pl.multiple_of((2 * ox + e) * ROWS + (1 - yy) * HR, HR), HR)]
        return remote(here, here, fws.at[g, m, e], fwr.at[g, m, e], twin)

    pl.semaphore_wait(barrier, 4)
    for g in range(PAIRS):
        for m in range(3):
            for e in range(2):
                w_cross(g, m, e).start()
        for m in range(3):
            w_partner(g, m).start()
            w_local(g, m).start()
    load_wo.start()

    load_x.wait()

    gain = gain_ref[...].astype(F32).reshape(1, D)

    def norm(i, _):
        rows = pl.ds(pl.multiple_of(s * OWN + i * 128, 128), 128)
        wide = a_s[rows, :].astype(F32)
        scale = lax.rsqrt(jnp.mean(wide * wide, -1, keepdims=True) + 1e-6)
        a_s[rows, :] = (wide * scale * gain).astype(BF)

    lax.fori_loop(0, OWN // 128, norm, None)

    def a_partner(j):
        here = a_s.at[_at(2 * s + j, BLK)]
        return remote(here, here, aps.at[j], apr.at[j], partner)

    def a_partner_in(j):
        here = a_s.at[_at(2 * (2 * x + 1 - c) + j, BLK)]
        return remote(here, here, aps.at[j], apr.at[j], partner)

    def a_cross(j):
        here = a_s.at[_at((4 * x + j) * 2 + c, HALF)]
        return remote(here, here, acs.at[j], acr.at[j], cross(c))

    def a_cross_in(j):
        here = a_s.at[_at((4 * ox + j) * 2 + c, HALF)]
        return remote(here, here, acs.at[j], acr.at[j], cross(c))

    def a_hand(j):
        here = a_s.at[_at((4 * ox + j) * 2 + c, HALF)]
        return remote(here, here, afs.at[j], afr.at[j], partner)

    def a_hand_in(j):
        here = a_s.at[_at((4 * ox + j) * 2 + 1 - c, HALF)]
        return remote(here, here, afs.at[j], afr.at[j], partner)

    def place(b):
        return pl.multiple_of(jnp.where(b // 4 == x, (b - 4 * x) * BLK, 4 * BLK), BLK)

    def project(b, g):
        rows, at_q = _at(b, BLK), pl.ds(place(b), BLK)
        a = a_s[rows, :]
        cr, sr = cos_ref[...], sin_ref[...]
        cb, sb = cosb_ref[pl.ds(b, 1), :], sinb_ref[pl.ds(b, 1), :]
        cos = cb * cr - sb * sr
        sin = sb * cr + cb * sr
        sin = jnp.where(lax.broadcasted_iota(jnp.int32, sin.shape, 1) < HEAD // 2, -sin, sin)

        def turned(t):
            t = t.astype(BF).astype(F32)
            return (t * cos + pltpu.roll(t, HEAD // 2, 1) * sin).astype(BF)

        q, k, v = (_dot(a, w_s[g, m], 1, 0) for m in range(3))
        for h in range(2):
            cut = slice(h * HEAD, (h + 1) * HEAD)
            q_s[2 * g + h, at_q, :] = turned(q[:, cut])
            k_s[2 * g + h, rows, :] = turned(k[:, cut])
            v_s[2 * g + h, :, rows] = v[:, cut].T.astype(BF)

    hidden = lax.broadcasted_iota(jnp.int32, (HALF, HALF), 0) > lax.broadcasted_iota(jnp.int32, (HALF, HALF), 1)

    def pieces(todo, ahead, lag):
        scores, weights = {}, {}
        for t in range(len(todo) + ahead + lag):
            if t < len(todo):
                h, at, n, first, keys, _ = todo[t][0]
                scores[t] = _dot(k_s[h, pl.ds(first, keys), :], q_s[h, pl.ds(at, n), :], 1, 1)
            if 0 <= t - ahead < len(todo):
                (h, at, n, first, keys, masked), (m, row, lanes), old = todo[t - ahead]
                e = scores.pop(t - ahead)
                if masked:
                    cut = jnp.where(hidden, 2 * NEG, e[-HALF:, :])
                    e = cut if keys == HALF else jnp.concatenate([e[:-HALF, :], cut], axis=0)
                top = e.max(axis=0, keepdims=True)
                keep = None
                if old:
                    before = row[:, lanes]
                    top = jnp.maximum(before, top)
                    keep = jnp.exp2((before - top) * E)
                row[:, lanes] = top
                weights[t - ahead] = jnp.exp2((e - top) * E).astype(BF), keep
            if 0 <= t - ahead - lag:
                (h, at, n, first, keys, masked), (m, row, lanes), old = todo[t - ahead - lag]
                p, keep = weights.pop(t - ahead - lag)
                got = _dot(jnp.concatenate([v_s[h, :, pl.ds(first, keys)], jnp.ones((8, keys), BF)], axis=0), p, 1, 0)
                mix_s[m, :, lanes] = mix_s[m, :, lanes] * keep + got if old else got

    def cut(i):
        return slice(i * HALF, (i + 1) * HALF)

    def state_out(g):
        return pltpu.make_async_copy(mix_s, st_hbm.at[g], st_sem.at[g])

    def state_in(j, g):
        return pltpu.make_async_copy(st_hbm.at[g, _at(j, 2)], mix_s.at[pl.ds(2 * g, 2)], st_sem.at[g])

    def near(g):
        todo = []
        for j in range(4):
            for h in range(2):
                for i in range(2):
                    piece = 2 * g + h, j * BLK + i * HALF, HALF, pl.multiple_of(4 * x * BLK, BLK), j * BLK + (i + 1) * HALF, True
                    todo.append((piece, (2 * j + h, top1_s.at[j, pl.ds(2 * g + h, 1)], cut(i)), False))
        pieces(todo, *NEAR)
        state_out(g).start()

    def diagonal(b, lead):
        todo = []
        for h in range(HEADS):
            for i in range(2):
                first = pl.multiple_of((b - lead) * BLK, BLK)
                piece = h, 4 * BLK + i * HALF, HALF, first, lead * BLK + (i + 1) * HALF, True
                todo.append((piece, (h, top_s.at[h : h + 1], cut(i)), False))
        pieces(todo, *DIAG)

    def whole(at_q, j):
        first = pl.multiple_of(2 * j * BLK, 2 * BLK)
        pieces([((h, at_q, BLK, first, 2 * BLK, False), (h, top_s.at[h : h + 1], slice(0, BLK)), True) for h in range(HEADS)], *WHOLE)

    def attend(at_q, steps):
        lax.fori_loop(0, steps, lambda j, _: whole(at_q, j), None)

    def normalize(at_q):
        for h in range(HEADS):
            got = mix_s[h, :HEAD, :] * (1 / mix_s[h, HEAD : HEAD + 1, :])
            q_s[h, pl.ds(at_q, BLK), :] = got.T.astype(BF)

    def output(at_q, slot):
        seen = jnp.concatenate([q_s[h, pl.ds(at_q, BLK), :] for h in range(HEADS)], axis=1)
        for n in range(0, D, PAIR):
            p_s[slot, :, n : n + PAIR] = _dot(seen, wo_s[:, n : n + PAIR], 1, 0)

    def hand(j):
        a_cross_in(j).wait_recv()
        a_hand(j).start()

    def arrive(g, m):
        for e in range(2):
            w_cross_in(g, m, e).wait_recv()
            w_twin(g, m, e).start()

    def near_weights(g):
        for m in range(3):
            w_local(g, m).wait()
            w_partner_in(g, m).wait_recv()

    def twin_weights(g):
        for m in range(3):
            for e in range(2):
                w_twin_in(g, m, e).wait_recv()

    def take(dev, g):
        for j in range(2):
            project(2 * dev + j, g)

    near_weights(0)
    for j in range(2):
        a_partner(j).start()
    for m in range(3):
        arrive(0, m)

    def weights(g, _):
        @pl.when(g > 0)
        def _():
            near_weights(g)

        twin_weights(g)

        def rows(i, _):
            @pl.when(g < PAIRS - 1)
            def _():
                for m in range(2):
                    @pl.when(i == m)
                    def _():
                        arrive(g + 1, m)

            @pl.when((g == 0) & (i == 1))
            def _():
                for j in range(2):
                    a_partner_in(j).wait_recv()

            take(jnp.where(i == 0, s, 2 * x + 1 - c), g)

        lax.fori_loop(0, 2, rows, None)

        @pl.when(g < PAIRS - 1)
        def _():
            arrive(g + 1, 2)

        @pl.when((g == 1) | (g == 2))
        def _():
            for j in range(2):
                a_cross(2 * (g - 1) + j).start()

        @pl.when(g == PAIRS - 1)
        def _():
            hand(0)

        @pl.when(g > 0)
        def _():
            state_out(g - 1).wait()

        near(g)

    lax.fori_loop(0, PAIRS, weights, None)
    load_wo.wait()

    def turn(t):
        return t % 2 * 2 + t // 2

    def to_owner(b, t):
        return remote(p_s.at[t % 2], accp_s.at[b % 2], os_.at[b % 2], or_.at[b % 2], partner)

    def to_half(b):
        return remote(p_s.at[0, _at(1 - c, HALF)], p_s.at[1, _at(b % 2, HALF)], hs.at[b % 2], hr.at[b % 2], partner)

    def to_cross(b):
        return remote(sendb_s.at[b % 2], recvb_s.at[b % 2, _at(c, HALF)], bs.at[b % 2], br.at[b % 2, c], (yy, b // 2))

    def finish_far(j):
        b = 4 * ox + j
        to_half(b).wait_send()
        to_half(b).wait_recv()

        @pl.when(j >= 2)
        def _():
            to_cross(b - 2).wait_send()

        def add(i, _):
            rows = pl.ds(pl.multiple_of(c * HALF + i * 64, 64), 64)
            sendb_s[b % 2, _at(i, 64), :] = (p_s[0, rows, :] + p_s[1, pl.ds(pl.multiple_of(b % 2 * HALF + i * 64, 64), 64), :]).astype(BF)

        lax.fori_loop(0, HALF // 64, add, None)
        to_cross(b).start()

    def y_out(n):
        return pltpu.make_async_copy(recvb_s.at[n], y_hbm.at[_at(n, BLK)], y_sem.at[n])

    def finish_own(t):
        b = 4 * x + turn(t)
        n = b % 2

        @pl.when(b // 2 == s)
        def _():
            for e in range(2):
                here = recvb_s.at[n, _at(e, HALF)]
                remote(here, here, bs.at[n], br.at[n, e], cross(e)).wait_recv()
            to_owner(b, t).wait_recv()

            def add(i, _):
                rows = _at(i, 64)
                total = p_s[t % 2, rows, :] + accp_s[n, rows, :] + recvb_s[n, rows, :].astype(F32)
                old = a_s[pl.ds(pl.multiple_of(b * BLK + i * 64, 64), 64), :].astype(F32)
                recvb_s[n, rows, :] = (old + total).astype(BF)

            lax.fori_loop(0, BLK // 64, add, None)
            y_out(n).start()

        @pl.when(b // 2 != s)
        def _():
            to_owner(b, t).wait_send()

    state_out(PAIRS - 1).wait()

    def far(j, _):
        b = 4 * ox + j
        a_hand_in(j).wait_recv()

        for g in range(PAIRS):
            project(b, g)

        @pl.when(j > 0)
        def _():
            finish_far(j - 1)

        @pl.when(b % 2 == 0)
        def _():
            diagonal(b, 0)

        @pl.when(b % 2 == 1)
        def _():
            diagonal(b, 1)

        attend(4 * BLK, b // 2)

        @pl.when(j < 3)
        def _():
            hand(j + 1)

        normalize(4 * BLK)
        output(4 * BLK, 0)
        to_half(b).start()

        @pl.when(j == 3)
        def _():
            for g in range(PAIRS):
                state_in(0, g).start()

    lax.fori_loop(0, 4, far, None)

    def own(t, _):
        j = turn(t)
        b = 4 * x + j
        for g in range(PAIRS):
            state_in(j, g).wait()
        top_s[...] = top1_s[j]
        at_q = pl.multiple_of(j * BLK, BLK)
        attend(at_q, 2 * x)
        normalize(at_q)

        @pl.when(t < 3)
        def _():
            for g in range(PAIRS):
                state_in(turn(t + 1), g).start()

        @pl.when(t == 0)
        def _():
            finish_far(3)

        output(at_q, t % 2)

        @pl.when(b // 2 != s)
        def _():
            to_owner(b, t).start()

        @pl.when(t == 1)
        def _():
            load_x.wait()

        @pl.when(t > 0)
        def _():
            finish_own(t - 1)

    for j in range(2):
        a_partner(j).wait_send()
    for j in range(4):
        a_cross(j).wait_send()
        a_hand(j).wait_send()
    load_x.start()
    for g in range(PAIRS):
        for m in range(3):
            w_partner(g, m).wait_send()
            for e in range(2):
                w_cross(g, m, e).wait_send()
                w_twin(g, m, e).wait_send()
    lax.fori_loop(0, 4, own, None)
    finish_own(3)
    for n in range(2):
        y_out(n).wait()
    for j in range(2, 4):
        to_cross(4 * ox + j).wait_send()


def tables(at):
    half = HEAD // 2
    angle = at[:, None] * float(THETA) ** (-np.arange(half) / half)
    return (np.concatenate([t, t], -1).astype(np.float32) for t in (np.cos(angle), np.sin(angle)))


def solution(mesh):
    def step(x, gain, wq, wk, wv, wo):
        cos, sin = tables(np.arange(BLK))
        cosb, sinb = tables(np.arange(NB) * BLK)
        hbm, vmem = pl.BlockSpec(memory_space=pl.ANY), pl.BlockSpec(memory_space=pltpu.VMEM)
        dma = pltpu.SemaphoreType.DMA
        y, _ = pl.pallas_call(
            kernel,
            out_shape=[jax.ShapeDtypeStruct((OWN, D), BF), jax.ShapeDtypeStruct((PAIRS, HEADS, HEAD + 8, BLK), F32)],
            in_specs=[hbm, vmem, hbm, hbm, hbm, hbm, vmem, vmem, vmem, vmem],
            out_specs=[hbm, hbm],
            scratch_shapes=[
                pltpu.VMEM((TOK, D), BF),
                pltpu.VMEM((PAIRS, 3, D, PAIR), BF),
                pltpu.VMEM((COLS, D), BF),
                pltpu.VMEM((HEADS, 5 * BLK, HEAD), BF),
                pltpu.VMEM((HEADS, TOK, HEAD), BF),
                pltpu.VMEM((HEADS, HEAD, TOK), BF),
                pltpu.VMEM((2, BLK, D), F32),
                pltpu.VMEM((2, BLK, D), F32),
                pltpu.VMEM((2, HALF, D), BF),
                pltpu.VMEM((2, BLK, D), BF),
                pltpu.VMEM((HEADS, HEAD + 8, BLK), F32),
                pltpu.VMEM((HEADS, BLK), F32),
                pltpu.VMEM((4, HEADS, BLK), F32),
                dma((2,)), dma((PAIRS,)), dma((PAIRS, 3)),
                dma((PAIRS, 3)), dma((PAIRS, 3)),
                dma((PAIRS, 3, 2)), dma((PAIRS, 3, 2)),
                dma((PAIRS, 3, 2)), dma((PAIRS, 3, 2)),
                dma((2,)), dma((2,)),
                dma((4,)), dma((4,)), dma((4,)), dma((4,)),
                dma((2,)), dma((2,)), dma((2,)), dma((2,)),
                dma((2,)), dma((2, 2)), dma((2,)),
            ],
            compiler_params=pltpu.CompilerParams(collective_id=0, has_side_effects=True, vmem_limit_bytes=67043328),
        )(x, gain, wq, wk, wv, wo, cos, sin, cosb, sinb)
        return y

    tokens, whole = P(("dp", "sp"), None), P("sp", None)
    return jax.shard_map(
        step,
        mesh=mesh,
        in_specs=(tokens, P(None), whole, whole, whole, whole),
        out_specs=tokens,
        check_vma=False,
    )
```

```python
import jax
import jax.numpy as jnp
import numpy as np
from jax import lax
from jax.experimental import pallas as pl
from jax.experimental.pallas import tpu as pltpu
from jax.sharding import PartitionSpec as P

HEAD = 128
THETA = 10000
NEG = -1e30
LOG2E = 1.4426950408889634
BF, F32 = jnp.bfloat16, jnp.float32

D = 1024
OWN = 1024
TOK = 4 * OWN
HEADS = 8
COLS = HEADS * HEAD
ROWS = D // 4
BLK = 512
HALF = BLK // 2
QUARTER = BLK // 4
NB = TOK // BLK
PAIR = 2 * HEAD
PAIRS = COLS // PAIR
HR = ROWS // 2
E = HEAD**-0.5 * LOG2E
NEAR, DIAG, WHOLE, STRIP = (2, 1), (3, 1), (1, 1), (3, 1)


def _dot(a, b, ca, cb):
    return lax.dot_general(a, b, (((ca,), (cb,)), ((), ())), preferred_element_type=F32)


def _at(i, n):
    return pl.ds(i * n if isinstance(i, int) else pl.multiple_of(i * n, n), n)


def kernel(x_hbm, gain_ref, wq_hbm, wk_hbm, wv_hbm, wo_hbm, cos_ref, sin_ref, cosb_ref, sinb_ref, y_hbm,
           st_hbm, a_s, w_s, wo_s, q_s, k_s, v_s, p_s, sendp_s, accp_s, sendb_s, recvb_s, mix_s, top_s, top1_s,
           loc_sem, st_sem, locw_sem, pws, pwr, cws, cwr, fws, fwr, aps, apr, acs, acr, afs, afr, os_, or_, hs, hr, bs, br, shs, shr, sbs, sbr, y_sem):
    yy, s = lax.axis_index("dp"), lax.axis_index("sp")
    x, c = s // 2, s % 2
    ox = 1 - x
    partner, twin = (yy, 2 * x + 1 - c), (1 - yy, s)
    cross = lambda e: (yy, 2 * ox + e)
    ws = (wq_hbm, wk_hbm, wv_hbm)

    def remote(src, dst, ssem, rsem, dev):
        return pltpu.make_async_remote_copy(src_ref=src, dst_ref=dst, send_sem=ssem, recv_sem=rsem, device_id=dev,
                                            device_id_type=pl.DeviceIdType.MESH)

    load_x = pltpu.make_async_copy(x_hbm, a_s.at[_at(s, OWN)], loc_sem.at[0])
    load_wo = pltpu.make_async_copy(wo_hbm, wo_s, loc_sem.at[1])
    load_x.start()
    barrier = pltpu.get_barrier_semaphore()
    for dev in (partner, twin, cross(0), cross(1)):
        pl.semaphore_signal(barrier, inc=1, device_id=dev, device_id_type=pl.DeviceIdType.MESH)

    def col(t, g):
        return pl.ds(pl.multiple_of(t * COLS + g * PAIR, PAIR), PAIR)

    def w_local(g, m):
        return pltpu.make_async_copy(ws[m].at[:, col(s, g)], w_s.at[g, m, _at(s, ROWS)], locw_sem.at[g, m])

    def w_partner(g, m):
        return remote(ws[m].at[:, col(2 * x + 1 - c, g)], w_s.at[g, m, _at(s, ROWS)], pws.at[g, m], pwr.at[g, m], partner)

    def w_partner_in(g, m):
        here = w_s.at[g, m, _at(2 * x + 1 - c, ROWS)]
        return remote(here, here, pws.at[g, m], pwr.at[g, m], partner)

    def w_cross(g, m, e):
        rows = _at(yy, HR)
        return remote(ws[m].at[rows, col(2 * ox + e, g)], w_s.at[g, m, pl.ds(pl.multiple_of(s * ROWS + yy * HR, HR), HR)],
                      cws.at[g, m, e], cwr.at[g, m, c], cross(e))

    def w_cross_in(g, m, e):
        here = w_s.at[g, m, pl.ds(pl.multiple_of((2 * ox + e) * ROWS + yy * HR, HR), HR)]
        return remote(here, here, cws.at[g, m, e], cwr.at[g, m, e], cross(e))

    def w_twin(g, m, e):
        here = w_s.at[g, m, pl.ds(pl.multiple_of((2 * ox + e) * ROWS + yy * HR, HR), HR)]
        return remote(here, here, fws.at[g, m, e], fwr.at[g, m, e], twin)

    def w_twin_in(g, m, e):
        here = w_s.at[g, m, pl.ds(pl.multiple_of((2 * ox + e) * ROWS + (1 - yy) * HR, HR), HR)]
        return remote(here, here, fws.at[g, m, e], fwr.at[g, m, e], twin)

    pl.semaphore_wait(barrier, 4)
    for g in range(PAIRS):
        for m in range(3):
            for e in range(2):
                w_cross(g, m, e).start()
        for m in range(3):
            w_partner(g, m).start()
            w_local(g, m).start()
    load_wo.start()

    load_x.wait()

    gain = gain_ref[...].astype(F32).reshape(1, D)

    def norm(i, _):
        rows = pl.ds(pl.multiple_of(s * OWN + i * 128, 128), 128)
        wide = a_s[rows, :].astype(F32)
        scale = lax.rsqrt(jnp.mean(wide * wide, -1, keepdims=True) + 1e-6)
        a_s[rows, :] = (wide * scale * gain).astype(BF)

    lax.fori_loop(0, OWN // 128, norm, None)

    def a_partner(j):
        here = a_s.at[_at(2 * s + j, BLK)]
        return remote(here, here, aps.at[j], apr.at[j], partner)

    def a_partner_in(j):
        here = a_s.at[_at(2 * (2 * x + 1 - c) + j, BLK)]
        return remote(here, here, aps.at[j], apr.at[j], partner)

    def a_cross(j):
        here = a_s.at[_at((4 * x + j) * 2 + c, HALF)]
        return remote(here, here, acs.at[j], acr.at[j], cross(c))

    def a_cross_in(j):
        here = a_s.at[_at((4 * ox + j) * 2 + c, HALF)]
        return remote(here, here, acs.at[j], acr.at[j], cross(c))

    def a_hand(j):
        here = a_s.at[_at((4 * ox + j) * 2 + c, HALF)]
        return remote(here, here, afs.at[j], afr.at[j], partner)

    def a_hand_in(j):
        here = a_s.at[_at((4 * ox + j) * 2 + 1 - c, HALF)]
        return remote(here, here, afs.at[j], afr.at[j], partner)

    def place(b):
        return pl.multiple_of(jnp.where(b // 4 == x, (b - 4 * x) * BLK, 4 * BLK), BLK)

    def project(b, g):
        rows, at_q = _at(b, BLK), pl.ds(place(b), BLK)
        a = a_s[rows, :]
        cr, sr = cos_ref[...], sin_ref[...]
        cb, sb = cosb_ref[pl.ds(b, 1), :], sinb_ref[pl.ds(b, 1), :]
        cos = cb * cr - sb * sr
        sin = sb * cr + cb * sr
        sin = jnp.where(lax.broadcasted_iota(jnp.int32, sin.shape, 1) < HEAD // 2, -sin, sin)

        def turned(t):
            t = t.astype(BF).astype(F32)
            return (t * cos + pltpu.roll(t, HEAD // 2, 1) * sin).astype(BF)

        q, k, v = (_dot(a, w_s[g, m], 1, 0) for m in range(3))
        for h in range(2):
            cut = slice(h * HEAD, (h + 1) * HEAD)
            q_s[2 * g + h, at_q, :] = turned(q[:, cut])
            k_s[2 * g + h, rows, :] = turned(k[:, cut])
            v_s[2 * g + h, :, rows] = v[:, cut].T.astype(BF)

    hidden = lax.broadcasted_iota(jnp.int32, (HALF, HALF), 0) > lax.broadcasted_iota(jnp.int32, (HALF, HALF), 1)

    def pieces(todo, ahead, lag):
        scores, weights = {}, {}
        for t in range(len(todo) + ahead + lag):
            if t < len(todo):
                h, at, n, first, keys, _ = todo[t][0]
                scores[t] = _dot(k_s[h, pl.ds(first, keys), :], q_s[h, pl.ds(at, n), :], 1, 1)
            if 0 <= t - ahead < len(todo):
                (h, at, n, first, keys, masked), (m, row, lanes), old = todo[t - ahead]
                e = scores.pop(t - ahead)
                if masked:
                    cut = jnp.where(hidden, 2 * NEG, e[-HALF:, :])
                    e = cut if keys == HALF else jnp.concatenate([e[:-HALF, :], cut], axis=0)
                top = e.max(axis=0, keepdims=True)
                keep = None
                if old:
                    before = row[:, lanes]
                    top = jnp.maximum(before, top)
                    keep = jnp.exp2((before - top) * E)
                row[:, lanes] = top
                weights[t - ahead] = jnp.exp2((e - top) * E).astype(BF), keep
            if 0 <= t - ahead - lag:
                (h, at, n, first, keys, masked), (m, row, lanes), old = todo[t - ahead - lag]
                p, keep = weights.pop(t - ahead - lag)
                got = _dot(jnp.concatenate([v_s[h, :, pl.ds(first, keys)], jnp.ones((8, keys), BF)], axis=0), p, 1, 0)
                mix_s[m, :, lanes] = mix_s[m, :, lanes] * keep + got if old else got

    def cut(i):
        return slice(i * HALF, (i + 1) * HALF)

    def state_out(g):
        return pltpu.make_async_copy(mix_s, st_hbm.at[g], st_sem.at[g])

    def state_in(j, g):
        return pltpu.make_async_copy(st_hbm.at[g, _at(j, 2)], mix_s.at[pl.ds(2 * g, 2)], st_sem.at[g])

    def near(g):
        todo = []
        for j in range(4):
            for h in range(2):
                for i in range(2):
                    piece = 2 * g + h, j * BLK + i * HALF, HALF, pl.multiple_of(4 * x * BLK, BLK), j * BLK + (i + 1) * HALF, True
                    todo.append((piece, (2 * j + h, top1_s.at[j, pl.ds(2 * g + h, 1)], cut(i)), False))
        pieces(todo, *NEAR)
        state_out(g).start()

    def diagonal(b, lead):
        todo = []
        for h in range(HEADS):
            for i in range(2):
                first = pl.multiple_of((b - lead) * BLK, BLK)
                piece = h, 4 * BLK + i * HALF, HALF, first, lead * BLK + (i + 1) * HALF, True
                todo.append((piece, (h, top_s.at[h : h + 1], cut(i)), False))
        pieces(todo, *DIAG)

    def whole(at_q, j):
        first = pl.multiple_of(2 * j * BLK, 2 * BLK)
        pieces([((h, at_q, BLK, first, 2 * BLK, False), (h, top_s.at[h : h + 1], slice(0, BLK)), True) for h in range(HEADS)], *WHOLE)

    def whole_strip(i, j):
        first = pl.multiple_of(2 * j * BLK, 2 * BLK)
        lanes, at = _at(i, HALF), pl.multiple_of(4 * BLK + i * HALF, HALF)
        pieces([((h, at, HALF, first, 2 * BLK, False), (h, top_s.at[h : h + 1], lanes), True) for h in range(HEADS)], *STRIP)

    def strip(i):
        lanes, at = _at(i, HALF), pl.ds(pl.multiple_of(4 * BLK + i * HALF, HALF), HALF)
        for h in range(HEADS):
            got = mix_s[h, :HEAD, lanes] * (1 / mix_s[h, HEAD : HEAD + 1, lanes])
            q_s[h, at, :] = got.T.astype(BF)
        seen = jnp.concatenate([q_s[h, at, :] for h in range(HEADS)], axis=1)
        for n in range(0, D, PAIR):
            p_s[0, lanes, n : n + PAIR] = _dot(seen, wo_s[:, n : n + PAIR], 1, 0)

    def attend(at_q, steps):
        lax.fori_loop(0, steps, lambda j, _: whole(at_q, j), None)

    def normalize(at_q):
        for h in range(HEADS):
            got = mix_s[h, :HEAD, :] * (1 / mix_s[h, HEAD : HEAD + 1, :])
            q_s[h, pl.ds(at_q, BLK), :] = got.T.astype(BF)

    def output(at_q, to, first=0, last=D):
        seen = jnp.concatenate([q_s[h, pl.ds(at_q, BLK), :] for h in range(HEADS)], axis=1)
        for n in range(first, last, PAIR):
            to[:, n : n + PAIR] = _dot(seen, wo_s[:, n : n + PAIR], 1, 0).astype(to.dtype)

    def hand(j):
        a_cross_in(j).wait_recv()
        a_hand(j).start()

    def arrive(g, m):
        for e in range(2):
            w_cross_in(g, m, e).wait_recv()
            w_twin(g, m, e).start()

    def near_weights(g):
        for m in range(3):
            w_local(g, m).wait()
            w_partner_in(g, m).wait_recv()

    def twin_weights(g):
        for m in range(3):
            for e in range(2):
                w_twin_in(g, m, e).wait_recv()

    def take(dev, g):
        for j in range(2):
            project(2 * dev + j, g)

    near_weights(0)
    for j in range(2):
        a_partner(j).start()
    for m in range(3):
        arrive(0, m)

    def weights(g, _):
        @pl.when(g > 0)
        def _():
            near_weights(g)

        @pl.when(g < PAIRS - 1)
        def _():
            arrive(g + 1, 0)

        twin_weights(g)

        def rows(i, _):
            @pl.when((g < PAIRS - 1) & (i == 1))
            def _():
                arrive(g + 1, 1)

            @pl.when((g == 0) & (i == 1))
            def _():
                for j in range(2):
                    a_partner_in(j).wait_recv()

            take(jnp.where(i == 0, s, 2 * x + 1 - c), g)

        lax.fori_loop(0, 2, rows, None)

        @pl.when(g < PAIRS - 1)
        def _():
            arrive(g + 1, 2)

        @pl.when((g == 1) | (g == 2))
        def _():
            for j in range(2):
                a_cross(2 * (g - 1) + j).start()

        @pl.when(g == PAIRS - 1)
        def _():
            hand(0)

        @pl.when(g > 0)
        def _():
            state_out(g - 1).wait()

        near(g)

    lax.fori_loop(0, PAIRS, weights, None)
    load_wo.wait()

    def turn(t):
        return t % 2 * 2 + t // 2

    def to_owner(b, i):
        columns = slice(i * D // 2, (i + 1) * D // 2)
        return remote(sendp_s.at[b % 2, :, columns], accp_s.at[b % 2, :, columns], os_.at[b % 2, i], or_.at[b % 2, i], partner)

    def to_half(b):
        return remote(p_s.at[0, _at(1 - c, HALF)], p_s.at[1, _at(b % 2, HALF)], hs.at[b % 2], hr.at[b % 2], partner)

    def to_cross(b):
        return remote(sendb_s.at[b % 2], recvb_s.at[b % 2, _at(c, HALF)], bs.at[b % 2], br.at[b % 2, c], (yy, b // 2))

    def finish_far(j):
        b = 4 * ox + j
        to_half(b).wait_send()
        to_half(b).wait_recv()

        @pl.when(j == 2)
        def _():
            to_cross(b - 2).wait_send()

        def add(i, _):
            rows = pl.ds(pl.multiple_of(c * HALF + i * 64, 64), 64)
            sendb_s[b % 2, _at(i, 64), :] = (p_s[0, rows, :] + p_s[1, pl.ds(pl.multiple_of(b % 2 * HALF + i * 64, 64), 64), :]).astype(BF)

        lax.fori_loop(0, HALF // 64, add, None)
        to_cross(b).start()

    LAST = 4 * ox + 3

    def strip_half(i):
        return remote(p_s.at[0, pl.ds(pl.multiple_of(i * HALF + (1 - c) * QUARTER, QUARTER), QUARTER)],
                      p_s.at[1, pl.ds(pl.multiple_of(HALF + i * QUARTER, QUARTER), QUARTER)], shs.at[i], shr.at[i], partner)

    def strip_cross(i):
        return remote(sendb_s.at[2, _at(i, QUARTER)], recvb_s.at[1, pl.ds(pl.multiple_of(i * HALF + c * QUARTER, QUARTER), QUARTER)],
                      sbs.at[i], sbr.at[i, c], (yy, LAST // 2))

    def finish_strip(i):
        strip_half(i).wait_send()
        strip_half(i).wait_recv()

        def add(k, _):
            rows = pl.ds(pl.multiple_of(i * HALF + c * QUARTER + k * 64, 64), 64)
            other = pl.ds(pl.multiple_of(HALF + i * QUARTER + k * 64, 64), 64)
            sendb_s[2, pl.ds(pl.multiple_of(i * QUARTER + k * 64, 64), 64), :] = (p_s[0, rows, :] + p_s[1, other, :]).astype(BF)

        lax.fori_loop(0, QUARTER // 64, add, None)
        strip_cross(i).start()

    def y_out(n, i):
        return pltpu.make_async_copy(recvb_s.at[n, _at(i, HALF)], y_hbm.at[_at(2 * n + i, HALF)], y_sem.at[n, i])

    def finish_own(t):
        b = 4 * x + turn(t)
        n = b % 2

        @pl.when(b // 2 == s)
        def _():
            @pl.when(b % 4 == 3)
            def _():
                for i in range(2):
                    for e in range(2):
                        here = recvb_s.at[1, pl.ds(i * HALF + e * QUARTER, QUARTER)]
                        remote(here, here, sbs.at[i], sbr.at[i, e], cross(e)).wait_recv()

            @pl.when(b % 4 != 3)
            def _():
                for e in range(2):
                    here = recvb_s.at[n, _at(e, HALF)]
                    remote(here, here, bs.at[n], br.at[n, e], cross(e)).wait_recv()

            for i in range(2):
                to_owner(b, i).wait_recv()

            def add(i, _):
                rows = _at(i, 64)
                total = p_s[n, rows, :] + accp_s[n, rows, :].astype(F32) + recvb_s[n, rows, :].astype(F32)
                old = a_s[pl.ds(pl.multiple_of(b * BLK + i * 64, 64), 64), :].astype(F32)
                recvb_s[n, rows, :] = (old + total).astype(BF)

            for i in range(2):
                lax.fori_loop(i * (HALF // 64), (i + 1) * (HALF // 64), add, None)
                y_out(n, i).start()

        @pl.when(b // 2 != s)
        def _():
            for i in range(2):
                to_owner(b, i).wait_send()

    def far_start(j):
        b = 4 * ox + j
        a_hand_in(j).wait_recv()
        for g in range(PAIRS):
            project(b, g)

        @pl.when(j > 0)
        def _():
            finish_far(j - 1)

        @pl.when(j == 0)
        def _():
            state_out(PAIRS - 1).wait()

        @pl.when(b % 2 == 0)
        def _():
            diagonal(b, 0)

        @pl.when(b % 2 == 1)
        def _():
            diagonal(b, 1)

    def far_end(j):
        hand(j + 1)
        normalize(4 * BLK)
        output(4 * BLK, p_s.at[0])
        to_half(4 * ox + j).start()

    def last_far():
        def one(i, _):
            whole_strip(i, LAST // 2 - 1)

            @pl.when(i == 1)
            def _():
                finish_strip(0)

            strip(i)
            strip_half(i).start()

        lax.fori_loop(0, 2, one, None)
        for g in range(PAIRS):
            state_in(0, g).start()

    def own_start(t):
        j = turn(t)
        for g in range(PAIRS):
            state_in(j, g).wait()
        top_s[...] = top1_s[j]

    def own_end(t):
        @pl.when(t == 0)
        def _():
            finish_strip(1)

        j = turn(t)
        b = 4 * x + j
        at_q = pl.multiple_of(j * BLK, BLK)
        normalize(at_q)

        @pl.when(t < 3)
        def _():
            for g in range(PAIRS):
                state_in(turn(t + 1), g).start()

        @pl.when(b // 2 == s)
        def _():
            output(at_q, p_s.at[b % 2])

        @pl.when(b // 2 != s)
        def _():
            for i in range(2):
                output(at_q, sendp_s.at[b % 2], i * D // 2, (i + 1) * D // 2)
                to_owner(b, i).start()

        @pl.when(t == 1)
        def _():
            load_x.wait()

        @pl.when(t > 1)
        def _():
            finish_own(t - 2)

    def sent():
        for j in range(2):
            a_partner(j).wait_send()
        for j in range(4):
            a_cross(j).wait_send()
            a_hand(j).wait_send()
        load_x.start()
        for g in range(PAIRS):
            for m in range(3):
                w_partner(g, m).wait_send()
                for e in range(2):
                    w_cross(g, m, e).wait_send()
                    w_twin(g, m, e).wait_send()

    def block(u, _):
        far = u < 4
        t = jnp.maximum(u - 4, 0)

        @pl.when(far)
        def _():
            far_start(u)

        @pl.when(u == 4)
        def _():
            sent()

        @pl.when(u >= 4)
        def _():
            own_start(t)

        at_q = pl.multiple_of(jnp.where(far, 4 * BLK, turn(t) * BLK), BLK)
        attend(at_q, jnp.where(far, (4 * ox + u) // 2 - u // 3, 2 * x))

        @pl.when(u < 3)
        def _():
            far_end(u)

        @pl.when(u == 3)
        def _():
            last_far()

        @pl.when(u >= 4)
        def _():
            own_end(t)

    lax.fori_loop(0, 8, block, None)
    finish_own(2)
    finish_own(3)
    for n in range(2):
        for i in range(2):
            y_out(n, i).wait()
    for b in (LAST - 2, LAST - 1):
        to_cross(b).wait_send()
    for i in range(2):
        strip_cross(i).wait_send()


def tables(at):
    half = HEAD // 2
    angle = at[:, None] * float(THETA) ** (-np.arange(half) / half)
    return (np.concatenate([t, t], -1).astype(np.float32) for t in (np.cos(angle), np.sin(angle)))


def solution(mesh):
    def step(x, gain, wq, wk, wv, wo):
        cos, sin = tables(np.arange(BLK))
        cosb, sinb = tables(np.arange(NB) * BLK)
        hbm, vmem = pl.BlockSpec(memory_space=pl.ANY), pl.BlockSpec(memory_space=pltpu.VMEM)
        dma = pltpu.SemaphoreType.DMA
        y, _ = pl.pallas_call(
            kernel,
            out_shape=[jax.ShapeDtypeStruct((OWN, D), BF), jax.ShapeDtypeStruct((PAIRS, HEADS, HEAD + 8, BLK), F32)],
            in_specs=[hbm, vmem, hbm, hbm, hbm, hbm, vmem, vmem, vmem, vmem],
            out_specs=[hbm, hbm],
            scratch_shapes=[
                pltpu.VMEM((TOK, D), BF),
                pltpu.VMEM((PAIRS, 3, D, PAIR), BF),
                pltpu.VMEM((COLS, D), BF),
                pltpu.VMEM((HEADS, 5 * BLK, HEAD), BF),
                pltpu.VMEM((HEADS, TOK, HEAD), BF),
                pltpu.VMEM((HEADS, HEAD, TOK), BF),
                pltpu.VMEM((2, BLK, D), F32),
                pltpu.VMEM((2, BLK, D), BF),
                pltpu.VMEM((2, BLK, D), BF),
                pltpu.VMEM((3, HALF, D), BF),
                pltpu.VMEM((2, BLK, D), BF),
                pltpu.VMEM((HEADS, HEAD + 8, BLK), F32),
                pltpu.VMEM((HEADS, BLK), F32),
                pltpu.VMEM((4, HEADS, BLK), F32),
                dma((2,)), dma((PAIRS,)), dma((PAIRS, 3)),
                dma((PAIRS, 3)), dma((PAIRS, 3)),
                dma((PAIRS, 3, 2)), dma((PAIRS, 3, 2)),
                dma((PAIRS, 3, 2)), dma((PAIRS, 3, 2)),
                dma((2,)), dma((2,)),
                dma((4,)), dma((4,)), dma((4,)), dma((4,)),
                dma((2, 2)), dma((2, 2)), dma((2,)), dma((2,)),
                dma((2,)), dma((2, 2)), dma((2,)), dma((2,)), dma((2,)), dma((2, 2)), dma((2, 2)),
            ],
            compiler_params=pltpu.CompilerParams(collective_id=0, has_side_effects=True, vmem_limit_bytes=67043328),
        )(x, gain, wq, wk, wv, wo, cos, sin, cosb, sinb)
        return y

    tokens, whole = P(("dp", "sp"), None), P("sp", None)
    return jax.shard_map(
        step,
        mesh=mesh,
        in_specs=(tokens, P(None), whole, whole, whole, whole),
        out_specs=tokens,
        check_vma=False,
    )
```

```python
import jax
import jax.numpy as jnp
import numpy as np
from jax import lax
from jax.experimental import pallas as pl
from jax.experimental.pallas import tpu as pltpu
from jax.sharding import PartitionSpec as P

HEAD = 128
THETA = 10000
NEG = -1e30
LOG2E = 1.4426950408889634
BF, F32 = jnp.bfloat16, jnp.float32

D = 1024
OWN = 1024
TOK = 4 * OWN
HEADS = 8
COLS = HEADS * HEAD
ROWS = D // 4
BLK = 512
HALF = BLK // 2
QUARTER = BLK // 4
NB = TOK // BLK
PAIR = 2 * HEAD
PAIRS = COLS // PAIR
HR = ROWS // 2
E = HEAD**-0.5 * LOG2E
NEAR, DIAG, WHOLE, STRIP = (2, 1), (3, 1), (1, 1), (3, 1)


def _dot(a, b, ca, cb):
    return lax.dot_general(a, b, (((ca,), (cb,)), ((), ())), preferred_element_type=F32)


def _at(i, n):
    return pl.ds(i * n if isinstance(i, int) else pl.multiple_of(i * n, n), n)


def kernel(x_hbm, gain_ref, wq_hbm, wk_hbm, wv_hbm, wo_hbm, cos_ref, sin_ref, cosb_ref, sinb_ref, y_hbm,
           st_hbm, a_s, w_s, wo_s, q_s, k_s, v_s, p_s, sendp_s, accp_s, sendb_s, recvb_s, mix_s, top_s, top1_s,
           loc_sem, st_sem, locw_sem, pws, pwr, cws, cwr, fws, fwr, aps, apr, acs, acr, afs, afr, os_, or_, hs, hr, bs, br, shs, shr, sbs, sbr, y_sem):
    yy, s = lax.axis_index("dp"), lax.axis_index("sp")
    x, c = s // 2, s % 2
    ox = 1 - x
    partner, twin = (yy, 2 * x + 1 - c), (1 - yy, s)
    cross = lambda e: (yy, 2 * ox + e)
    ws = (wq_hbm, wk_hbm, wv_hbm)

    def remote(src, dst, ssem, rsem, dev):
        return pltpu.make_async_remote_copy(src_ref=src, dst_ref=dst, send_sem=ssem, recv_sem=rsem, device_id=dev,
                                            device_id_type=pl.DeviceIdType.MESH)

    load_x = pltpu.make_async_copy(x_hbm, a_s.at[_at(s, OWN)], loc_sem.at[0])
    load_wo = pltpu.make_async_copy(wo_hbm, wo_s, loc_sem.at[1])
    load_x.start()
    barrier = pltpu.get_barrier_semaphore()
    for dev in (partner, twin, cross(0), cross(1)):
        pl.semaphore_signal(barrier, inc=1, device_id=dev, device_id_type=pl.DeviceIdType.MESH)

    def col(t, g):
        return pl.ds(pl.multiple_of(t * COLS + g * PAIR, PAIR), PAIR)

    def w_local(g, m):
        return pltpu.make_async_copy(ws[m].at[:, col(s, g)], w_s.at[g, m, _at(s, ROWS)], locw_sem.at[g, m])

    def w_partner(g, m):
        return remote(ws[m].at[:, col(2 * x + 1 - c, g)], w_s.at[g, m, _at(s, ROWS)], pws.at[g, m], pwr.at[g, m], partner)

    def w_partner_in(g, m):
        here = w_s.at[g, m, _at(2 * x + 1 - c, ROWS)]
        return remote(here, here, pws.at[g, m], pwr.at[g, m], partner)

    def w_cross(g, m, e):
        rows = _at(yy, HR)
        return remote(ws[m].at[rows, col(2 * ox + e, g)], w_s.at[g, m, pl.ds(pl.multiple_of(s * ROWS + yy * HR, HR), HR)],
                      cws.at[g, m, e], cwr.at[g, m, c], cross(e))

    def w_cross_in(g, m, e):
        here = w_s.at[g, m, pl.ds(pl.multiple_of((2 * ox + e) * ROWS + yy * HR, HR), HR)]
        return remote(here, here, cws.at[g, m, e], cwr.at[g, m, e], cross(e))

    def w_twin(g, m, e):
        here = w_s.at[g, m, pl.ds(pl.multiple_of((2 * ox + e) * ROWS + yy * HR, HR), HR)]
        return remote(here, here, fws.at[g, m, e], fwr.at[g, m, e], twin)

    def w_twin_in(g, m, e):
        here = w_s.at[g, m, pl.ds(pl.multiple_of((2 * ox + e) * ROWS + (1 - yy) * HR, HR), HR)]
        return remote(here, here, fws.at[g, m, e], fwr.at[g, m, e], twin)

    pl.semaphore_wait(barrier, 4)
    for g in range(PAIRS):
        for m in range(3):
            for e in range(2):
                w_cross(g, m, e).start()
        for m in range(3):
            w_partner(g, m).start()
            w_local(g, m).start()
    load_wo.start()

    load_x.wait()

    gain = gain_ref[...].astype(F32).reshape(1, D)

    def norm(i, _):
        rows = pl.ds(pl.multiple_of(s * OWN + i * 128, 128), 128)
        wide = a_s[rows, :].astype(F32)
        scale = lax.rsqrt(jnp.mean(wide * wide, -1, keepdims=True) + 1e-6)
        a_s[rows, :] = (wide * scale * gain).astype(BF)

    lax.fori_loop(0, OWN // 128, norm, None)

    def a_partner(j):
        here = a_s.at[_at(2 * s + j, BLK)]
        return remote(here, here, aps.at[j], apr.at[j], partner)

    def a_partner_in(j):
        here = a_s.at[_at(2 * (2 * x + 1 - c) + j, BLK)]
        return remote(here, here, aps.at[j], apr.at[j], partner)

    def a_cross(j):
        here = a_s.at[_at((4 * x + j) * 2 + c, HALF)]
        return remote(here, here, acs.at[j], acr.at[j], cross(c))

    def a_cross_in(j):
        here = a_s.at[_at((4 * ox + j) * 2 + c, HALF)]
        return remote(here, here, acs.at[j], acr.at[j], cross(c))

    def a_hand(j):
        here = a_s.at[_at((4 * ox + j) * 2 + c, HALF)]
        return remote(here, here, afs.at[j], afr.at[j], partner)

    def a_hand_in(j):
        here = a_s.at[_at((4 * ox + j) * 2 + 1 - c, HALF)]
        return remote(here, here, afs.at[j], afr.at[j], partner)

    def place(b):
        return pl.multiple_of(jnp.where(b // 4 == x, (b - 4 * x) * BLK, 4 * BLK), BLK)

    def project(b, g):
        rows, at_q = _at(b, BLK), pl.ds(place(b), BLK)
        a = a_s[rows, :]
        cr, sr = cos_ref[...], sin_ref[...]
        cb, sb = cosb_ref[pl.ds(b, 1), :], sinb_ref[pl.ds(b, 1), :]
        cos = cb * cr - sb * sr
        sin = sb * cr + cb * sr
        sin = jnp.where(lax.broadcasted_iota(jnp.int32, sin.shape, 1) < HEAD // 2, -sin, sin)

        def turned(t):
            t = t.astype(BF).astype(F32)
            return (t * cos + pltpu.roll(t, HEAD // 2, 1) * sin).astype(BF)

        q, k, v = (_dot(a, w_s[g, m], 1, 0) for m in range(3))
        for h in range(2):
            cut = slice(h * HEAD, (h + 1) * HEAD)
            q_s[2 * g + h, at_q, :] = turned(q[:, cut])
            k_s[2 * g + h, rows, :] = turned(k[:, cut])
            v_s[2 * g + h, :, rows] = v[:, cut].T.astype(BF)

    hidden = lax.broadcasted_iota(jnp.int32, (HALF, HALF), 0) > lax.broadcasted_iota(jnp.int32, (HALF, HALF), 1)

    def pieces(todo, ahead, lag):
        scores, weights = {}, {}
        for t in range(len(todo) + ahead + lag):
            if t < len(todo):
                h, at, n, first, keys, _ = todo[t][0]
                scores[t] = _dot(k_s[h, pl.ds(first, keys), :], q_s[h, pl.ds(at, n), :], 1, 1)
            if 0 <= t - ahead < len(todo):
                (h, at, n, first, keys, masked), (m, row, lanes), old = todo[t - ahead]
                e = scores.pop(t - ahead)
                if masked:
                    cut = jnp.where(hidden, 2 * NEG, e[-HALF:, :])
                    e = cut if keys == HALF else jnp.concatenate([e[:-HALF, :], cut], axis=0)
                top = e.max(axis=0, keepdims=True)
                keep = None
                if old:
                    before = row[:, lanes]
                    top = jnp.maximum(before, top)
                    keep = jnp.exp2((before - top) * E)
                row[:, lanes] = top
                weights[t - ahead] = jnp.exp2((e - top) * E).astype(BF), keep
            if 0 <= t - ahead - lag:
                (h, at, n, first, keys, masked), (m, row, lanes), old = todo[t - ahead - lag]
                p, keep = weights.pop(t - ahead - lag)
                got = _dot(jnp.concatenate([v_s[h, :, pl.ds(first, keys)], jnp.ones((8, keys), BF)], axis=0), p, 1, 0)
                mix_s[m, :, lanes] = mix_s[m, :, lanes] * keep + got if old else got

    def cut(i):
        return slice(i * HALF, (i + 1) * HALF)

    def state_out(g):
        return pltpu.make_async_copy(mix_s, st_hbm.at[g], st_sem.at[g])

    def state_in(j, g):
        return pltpu.make_async_copy(st_hbm.at[g, _at(j, 2)], mix_s.at[pl.ds(2 * g, 2)], st_sem.at[g])

    def near(g):
        todo = []
        for j in range(4):
            for h in range(2):
                for i in range(2):
                    piece = 2 * g + h, j * BLK + i * HALF, HALF, pl.multiple_of(4 * x * BLK, BLK), j * BLK + (i + 1) * HALF, True
                    todo.append((piece, (2 * j + h, top1_s.at[j, pl.ds(2 * g + h, 1)], cut(i)), False))
        pieces(todo, *NEAR)
        state_out(g).start()

    def diagonal(b, lead):
        todo = []
        for h in range(HEADS):
            for i in range(2):
                first = pl.multiple_of((b - lead) * BLK, BLK)
                piece = h, 4 * BLK + i * HALF, HALF, first, lead * BLK + (i + 1) * HALF, True
                todo.append((piece, (h, top_s.at[h : h + 1], cut(i)), False))
        pieces(todo, *DIAG)

    def whole(at_q, j):
        first = pl.multiple_of(2 * j * BLK, 2 * BLK)
        pieces([((h, at_q, BLK, first, 2 * BLK, False), (h, top_s.at[h : h + 1], slice(0, BLK)), True) for h in range(HEADS)], *WHOLE)

    def whole_strip(i, j):
        first = pl.multiple_of(2 * j * BLK, 2 * BLK)
        lanes, at = _at(i, HALF), pl.multiple_of(4 * BLK + i * HALF, HALF)
        pieces([((h, at, HALF, first, 2 * BLK, False), (h, top_s.at[h : h + 1], lanes), True) for h in range(HEADS)], *STRIP)

    def strip(i):
        lanes, at = _at(i, HALF), pl.ds(pl.multiple_of(4 * BLK + i * HALF, HALF), HALF)
        for h in range(HEADS):
            got = mix_s[h, :HEAD, lanes] * (1 / mix_s[h, HEAD : HEAD + 1, lanes])
            q_s[h, at, :] = got.T.astype(BF)
        seen = jnp.concatenate([q_s[h, at, :] for h in range(HEADS)], axis=1)
        for n in range(0, D, PAIR):
            p_s[0, lanes, n : n + PAIR] = _dot(seen, wo_s[:, n : n + PAIR], 1, 0)

    def attend(at_q, steps):
        lax.fori_loop(0, steps, lambda j, _: whole(at_q, j), None)

    def normalize(at_q):
        for h in range(HEADS):
            got = mix_s[h, :HEAD, :] * (1 / mix_s[h, HEAD : HEAD + 1, :])
            q_s[h, pl.ds(at_q, BLK), :] = got.T.astype(BF)

    def output(at_q, to, first=0, last=D):
        seen = jnp.concatenate([q_s[h, pl.ds(at_q, BLK), :] for h in range(HEADS)], axis=1)
        for n in range(first, last, PAIR):
            to[:, n : n + PAIR] = _dot(seen, wo_s[:, n : n + PAIR], 1, 0).astype(to.dtype)

    def hand(j):
        a_cross_in(j).wait_recv()
        a_hand(j).start()

    def arrive(g, m):
        for e in range(2):
            w_cross_in(g, m, e).wait_recv()
            w_twin(g, m, e).start()

    def near_weights(g):
        for m in range(3):
            w_local(g, m).wait()
            w_partner_in(g, m).wait_recv()

    def twin_weights(g):
        for m in range(3):
            for e in range(2):
                w_twin_in(g, m, e).wait_recv()

    def take(dev, g):
        for j in range(2):
            project(2 * dev + j, g)

    near_weights(0)
    for j in range(2):
        a_partner(j).start()
    for m in range(3):
        arrive(0, m)

    def weights(g, _):
        @pl.when(g > 0)
        def _():
            near_weights(g)

        @pl.when(g < PAIRS - 1)
        def _():
            arrive(g + 1, 0)

        twin_weights(g)

        def rows(i, _):
            @pl.when((g < PAIRS - 1) & (i == 1))
            def _():
                arrive(g + 1, 1)

            @pl.when((g == 0) & (i == 1))
            def _():
                for j in range(2):
                    a_partner_in(j).wait_recv()

            take(jnp.where(i == 0, s, 2 * x + 1 - c), g)

        lax.fori_loop(0, 2, rows, None)

        @pl.when(g < PAIRS - 1)
        def _():
            arrive(g + 1, 2)

        @pl.when((g == 1) | (g == 2))
        def _():
            for j in range(2):
                a_cross(2 * (g - 1) + j).start()

        @pl.when(g == PAIRS - 1)
        def _():
            hand(0)

        @pl.when(g > 0)
        def _():
            state_out(g - 1).wait()

        near(g)

    lax.fori_loop(0, PAIRS, weights, None)
    load_wo.wait()

    def turn(t):
        return t % 2 * 2 + t // 2

    def to_owner(b, i):
        columns = slice(i * D // 2, (i + 1) * D // 2)
        return remote(sendp_s.at[b % 2, :, columns], accp_s.at[b % 2, :, columns], os_.at[b % 2, i], or_.at[b % 2, i], partner)

    def to_half(b):
        return remote(p_s.at[0, _at(1 - c, HALF)], p_s.at[1, _at(b % 2, HALF)], hs.at[b % 2], hr.at[b % 2], partner)

    def to_cross(b):
        return remote(sendb_s.at[b % 4], recvb_s.at[b % 2, _at(c, HALF)], bs.at[b % 4], br.at[b % 2, c], (yy, b // 2))

    def finish_far(j):
        b = 4 * ox + j
        to_half(b).wait_send()
        to_half(b).wait_recv()

        def add(i, _):
            rows = pl.ds(pl.multiple_of(c * HALF + i * 64, 64), 64)
            sendb_s[b % 4, _at(i, 64), :] = (p_s[0, rows, :] + p_s[1, pl.ds(pl.multiple_of(b % 2 * HALF + i * 64, 64), 64), :]).astype(BF)

        lax.fori_loop(0, HALF // 64, add, None)
        to_cross(b).start()

    LAST = 4 * ox + 3
    SPLIT = jnp.maximum(LAST // 2 - 2, 0)

    def strip_half(i):
        return remote(p_s.at[0, pl.ds(pl.multiple_of(i * HALF + (1 - c) * QUARTER, QUARTER), QUARTER)],
                      p_s.at[1, pl.ds(pl.multiple_of(HALF + i * QUARTER, QUARTER), QUARTER)], shs.at[i], shr.at[i], partner)

    def strip_cross(i):
        return remote(sendb_s.at[3, _at(i, QUARTER)], recvb_s.at[1, pl.ds(pl.multiple_of(i * HALF + c * QUARTER, QUARTER), QUARTER)],
                      sbs.at[i], sbr.at[i, c], (yy, LAST // 2))

    def finish_strip(i):
        strip_half(i).wait_send()
        strip_half(i).wait_recv()

        def add(k, _):
            rows = pl.ds(pl.multiple_of(i * HALF + c * QUARTER + k * 64, 64), 64)
            other = pl.ds(pl.multiple_of(HALF + i * QUARTER + k * 64, 64), 64)
            sendb_s[3, pl.ds(pl.multiple_of(i * QUARTER + k * 64, 64), 64), :] = (p_s[0, rows, :] + p_s[1, other, :]).astype(BF)

        lax.fori_loop(0, QUARTER // 64, add, None)
        strip_cross(i).start()

    def y_out(n, i):
        return pltpu.make_async_copy(recvb_s.at[n, _at(i, HALF)], y_hbm.at[_at(2 * n + i, HALF)], y_sem.at[n, i])

    def finish_own(t):
        b = 4 * x + turn(t)
        n = b % 2

        @pl.when(b // 2 == s)
        def _():
            @pl.when(b % 4 == 3)
            def _():
                for i in range(2):
                    for e in range(2):
                        here = recvb_s.at[1, pl.ds(i * HALF + e * QUARTER, QUARTER)]
                        remote(here, here, sbs.at[i], sbr.at[i, e], cross(e)).wait_recv()

            @pl.when(b % 4 != 3)
            def _():
                for e in range(2):
                    here = recvb_s.at[n, _at(e, HALF)]
                    remote(here, here, bs.at[n], br.at[n, e], cross(e)).wait_recv()

            for i in range(2):
                to_owner(b, i).wait_recv()

            def add(i, _):
                rows = _at(i, 64)
                total = p_s[n, rows, :] + accp_s[n, rows, :].astype(F32) + recvb_s[n, rows, :].astype(F32)
                old = a_s[pl.ds(pl.multiple_of(b * BLK + i * 64, 64), 64), :].astype(F32)
                recvb_s[n, rows, :] = (old + total).astype(BF)

            for i in range(2):
                lax.fori_loop(i * (HALF // 64), (i + 1) * (HALF // 64), add, None)
                y_out(n, i).start()

        @pl.when(b // 2 != s)
        def _():
            for i in range(2):
                to_owner(b, i).wait_send()

    def far_start(j):
        b = 4 * ox + j
        a_hand_in(j).wait_recv()
        for g in range(PAIRS):
            project(b, g)

        @pl.when(j > 0)
        def _():
            finish_far(j - 1)

        @pl.when(j == 0)
        def _():
            state_out(PAIRS - 1).wait()

        @pl.when(b % 2 == 0)
        def _():
            diagonal(b, 0)

        @pl.when(b % 2 == 1)
        def _():
            diagonal(b, 1)

    def far_end(j):
        hand(j + 1)
        normalize(4 * BLK)
        output(4 * BLK, p_s.at[0])
        to_half(4 * ox + j).start()

    def last_far():
        def one(i, _):
            def step(j, _):
                whole_strip(i, j)

                @pl.when((i == 1) & (j == SPLIT))
                def _():
                    finish_strip(0)

            lax.fori_loop(SPLIT, LAST // 2, step, None)
            strip(i)
            strip_half(i).start()

        lax.fori_loop(0, 2, one, None)
        for g in range(PAIRS):
            state_in(0, g).start()

    def own_start(t):
        j = turn(t)
        for g in range(PAIRS):
            state_in(j, g).wait()
        top_s[...] = top1_s[j]

    def own_end(t):
        @pl.when(t == 0)
        def _():
            finish_strip(1)

        j = turn(t)
        b = 4 * x + j
        at_q = pl.multiple_of(j * BLK, BLK)
        normalize(at_q)

        @pl.when(t < 3)
        def _():
            for g in range(PAIRS):
                state_in(turn(t + 1), g).start()

        @pl.when(b // 2 == s)
        def _():
            output(at_q, p_s.at[b % 2])

        @pl.when(b // 2 != s)
        def _():
            for i in range(2):
                output(at_q, sendp_s.at[b % 2], i * D // 2, (i + 1) * D // 2)
                to_owner(b, i).start()

        @pl.when(t == 1)
        def _():
            load_x.wait()

        @pl.when(t > 1)
        def _():
            finish_own(t - 2)

    def sent():
        for j in range(2):
            a_partner(j).wait_send()
        for j in range(4):
            a_cross(j).wait_send()
            a_hand(j).wait_send()
        load_x.start()
        for g in range(PAIRS):
            for m in range(3):
                w_partner(g, m).wait_send()
                for e in range(2):
                    w_cross(g, m, e).wait_send()
                    w_twin(g, m, e).wait_send()

    def block(u, _):
        far = u < 4
        t = jnp.maximum(u - 4, 0)

        @pl.when(far)
        def _():
            far_start(u)

        @pl.when(u == 4)
        def _():
            sent()

        @pl.when(u >= 4)
        def _():
            own_start(t)

        at_q = pl.multiple_of(jnp.where(far, 4 * BLK, turn(t) * BLK), BLK)
        attend(at_q, jnp.where(far, jnp.where(u == 3, SPLIT, (4 * ox + u) // 2), 2 * x))

        @pl.when(u < 3)
        def _():
            far_end(u)

        @pl.when(u == 3)
        def _():
            last_far()

        @pl.when(u >= 4)
        def _():
            own_end(t)

    lax.fori_loop(0, 8, block, None)
    finish_own(2)
    finish_own(3)
    for n in range(2):
        for i in range(2):
            y_out(n, i).wait()
    for b in (LAST - 3, LAST - 2, LAST - 1):
        to_cross(b).wait_send()
    for i in range(2):
        strip_cross(i).wait_send()


def tables(at):
    half = HEAD // 2
    angle = at[:, None] * float(THETA) ** (-np.arange(half) / half)
    return (np.concatenate([t, t], -1).astype(np.float32) for t in (np.cos(angle), np.sin(angle)))


def solution(mesh):
    def step(x, gain, wq, wk, wv, wo):
        cos, sin = tables(np.arange(BLK))
        cosb, sinb = tables(np.arange(NB) * BLK)
        hbm, vmem = pl.BlockSpec(memory_space=pl.ANY), pl.BlockSpec(memory_space=pltpu.VMEM)
        dma = pltpu.SemaphoreType.DMA
        y, _ = pl.pallas_call(
            kernel,
            out_shape=[jax.ShapeDtypeStruct((OWN, D), BF), jax.ShapeDtypeStruct((PAIRS, HEADS, HEAD + 8, BLK), F32)],
            in_specs=[hbm, vmem, hbm, hbm, hbm, hbm, vmem, vmem, vmem, vmem],
            out_specs=[hbm, hbm],
            scratch_shapes=[
                pltpu.VMEM((TOK, D), BF),
                pltpu.VMEM((PAIRS, 3, D, PAIR), BF),
                pltpu.VMEM((COLS, D), BF),
                pltpu.VMEM((HEADS, 5 * BLK, HEAD), BF),
                pltpu.VMEM((HEADS, TOK, HEAD), BF),
                pltpu.VMEM((HEADS, HEAD, TOK), BF),
                pltpu.VMEM((2, BLK, D), F32),
                pltpu.VMEM((2, BLK, D), BF),
                pltpu.VMEM((2, BLK, D), BF),
                pltpu.VMEM((4, HALF, D), BF),
                pltpu.VMEM((2, BLK, D), BF),
                pltpu.VMEM((HEADS, HEAD + 8, BLK), F32),
                pltpu.VMEM((HEADS, BLK), F32),
                pltpu.VMEM((4, HEADS, BLK), F32),
                dma((2,)), dma((PAIRS,)), dma((PAIRS, 3)),
                dma((PAIRS, 3)), dma((PAIRS, 3)),
                dma((PAIRS, 3, 2)), dma((PAIRS, 3, 2)),
                dma((PAIRS, 3, 2)), dma((PAIRS, 3, 2)),
                dma((2,)), dma((2,)),
                dma((4,)), dma((4,)), dma((4,)), dma((4,)),
                dma((2, 2)), dma((2, 2)), dma((2,)), dma((2,)),
                dma((3,)), dma((2, 2)), dma((2,)), dma((2,)), dma((2,)), dma((2, 2)), dma((2, 2)),
            ],
            compiler_params=pltpu.CompilerParams(collective_id=0, has_side_effects=True, vmem_limit_bytes=67043328),
        )(x, gain, wq, wk, wv, wo, cos, sin, cosb, sinb)
        return y

    tokens, whole = P(("dp", "sp"), None), P("sp", None)
    return jax.shard_map(
        step,
        mesh=mesh,
        in_specs=(tokens, P(None), whole, whole, whole, whole),
        out_specs=tokens,
        check_vma=False,
    )
```
